32 devices in a mesh: grp: 4 (over y, x), dev: 8 (over z, core).
Axes of the slice: x: 2, y: 2, z: 4, core: 2. Of those that a mesh axis runs over, the one named last changes fastest.
Arguments:
- source_id: int32 [524288], P(('grp', 'dev')), may hold values from 0 to 4095, as said below
- slot: int32 [524288], P(('grp', 'dev')), may hold values from 0 to 127, as said below
- owner: int32 [4096], replicated, may hold values from 0 to 4095, as said below
- counts: int32 [4096], P(('grp', 'dev')), may hold values from 1 to 128, as said below
- partials: float32 [5, 524288], P(None, ('grp', 'dev')), may hold values from -6 to 6
- residual: float32 [524288], P(('grp', 'dev')), may hold values from -6 to 6
- weight: float32 [524288], P(('grp', 'dev')), may hold values from 0.3 to 9
- prior: float32 [5, 4096], P(None, ('grp', 'dev')), may hold values from 0.5 to 4
Outputs:
- updates: float32 [5, 4096], P(None, ('grp', 'dev'))
- standardized: float32 [524288], P(('grp', 'dev'))
- norm: float32 [], replicated
The draws below stay inside these ranges and needn't reach their ends.
Inputs may be any that keep to these rules, and one draw needn't show every extreme that they name: A permutation: source s stands at owner position owner[s], and position p belongs to device p // 128. `source_id`: the rows of one device stand in 32 aligned blocks of 512 rows; block k holds only rows whose source's owner position lies in device k's range. Over all rows, each pair of a source and a slot below 128 appears exactly once. A row is an observation when its slot is below its source's count, else padding. Each device's block of counts holds 128 at least once.
All inputs are finite; a program needn't handle non-finite values.
Results may differ from the reference program's by a relative error of at most 0.0003.
Values sent between devices are 32-bit elements; how exact they have to be, the bound alone decides.
A program may use at most 64 MiB of HBM per device.

```python
import math
import jax
import jax.numpy as jnp
from jax import lax

PARAMS = 5
PAD = 128
SRC_DEV = 128
SOURCES = 4096
ROWS_DEV = 16384
ROWS_ALL = 524288
CAP = 512
N_GRP = 4
N_DEV = 8


def row_layout(key):
    base_key = jax.random.fold_in(key, 7001)
    devices_all = N_GRP * N_DEV
    placing = jax.random.permutation(jax.random.fold_in(base_key, 1), SOURCES).astype(jnp.int32)
    at_position = jnp.argsort(placing, stable=True).astype(jnp.int32)

    def owner_cells(owner_k):
        return jax.random.permutation(jax.random.fold_in(base_key, 1000 + owner_k), ROWS_DEV).astype(jnp.int32)
    cell_map = jax.vmap(owner_cells)(jnp.arange(devices_all, dtype=jnp.int32))
    cell_map = cell_map.reshape(devices_all, devices_all, CAP).transpose(1, 0, 2)
    owner_of = jnp.broadcast_to(jnp.arange(devices_all, dtype=jnp.int32)[None, :, None], cell_map.shape)
    position = owner_of * SRC_DEV + cell_map // PAD
    source_ids = at_position[position.reshape(-1)]
    slots = (cell_map % PAD).reshape(-1)
    return (placing, source_ids, slots)


def draw_owner(key, part):
    return row_layout(key)[0]


def draw_source_id(key, part):
    return row_layout(key)[1]


def draw_slot(key, part):
    return row_layout(key)[2]


def draw_counts(key, part):
    base_key = jax.random.fold_in(key, 7002)
    first_try = jax.random.randint(jax.random.fold_in(base_key, 1), (SOURCES,), 1, PAD + 1)
    second_try = jax.random.randint(jax.random.fold_in(base_key, 2), (SOURCES,), 1, PAD + 1)
    few_obs = jax.random.randint(jax.random.fold_in(base_key, 3), (SOURCES,), 1, PAD // 8 + 1)
    pick_low = jax.random.randint(jax.random.fold_in(base_key, 4), (SOURCES,), 0, 4) == 0
    result = jnp.where(pick_low, few_obs, jnp.maximum(first_try, second_try))
    full_slot = jax.random.randint(jax.random.fold_in(base_key, 5), (N_GRP * N_DEV,), 0, SRC_DEV)
    spots = jnp.arange(SOURCES, dtype=jnp.int32)
    result = jnp.where(spots % SRC_DEV == full_slot[spots // SRC_DEV], PAD, result)
    return result.astype(jnp.int32)


def draw_weight(key, part):
    row_device = jnp.arange(ROWS_ALL, dtype=jnp.int32) // ROWS_DEV
    rising = 1.0 + 2.0 * row_device.astype(jnp.float32) / max(N_GRP * N_DEV - 1, 1)
    spread = jnp.exp(jax.random.uniform(key, (ROWS_ALL,), jnp.float32, math.log(0.3), math.log(3.0)))
    return (spread * rising).astype(jnp.float32)


def steps_of(stream_key, shape, cuts, smallest, high):
    level, own = 1.0, jax.random.fold_in(stream_key, 6)
    for dim, blocks in cuts:
        heights = jnp.exp(jax.random.uniform(jax.random.fold_in(own, dim), (blocks,), jnp.float32, smallest / len(cuts), high / len(cuts)))
        level = level * jnp.repeat(heights, shape[dim] // blocks).reshape([-1 if axis == dim else 1 for axis in range(len(shape))])
    return level


def gaussian(own_key, extent, width, bound, pieces=(), kind=jnp.bfloat16):
    factor_of = steps_of(own_key, extent, pieces, -0.22, 0.18) if pieces else 1.0
    values = jax.random.normal(own_key, extent, jnp.float32) * width * factor_of
    return jnp.minimum(jnp.maximum(values, -bound), bound).astype(kind)


def setup_inputs(seed: int = 0) -> dict:
    streams_of = jax.random.split(jax.random.key(seed), 9)
    source_id = draw_source_id(jax.random.fold_in(streams_of[8], 71), 0)
    slot = draw_slot(jax.random.fold_in(streams_of[8], 71), 0)
    owner = draw_owner(jax.random.fold_in(streams_of[8], 71), 0)
    counts = draw_counts(jax.random.fold_in(streams_of[8], 71), 0)
    partials = gaussian(streams_of[4], (PARAMS, ROWS_ALL), 1.0, 6.0, ((1, 32),), jnp.float32)
    residual = gaussian(streams_of[5], (ROWS_ALL,), 1.0, 6.0, ((0, 32),), jnp.float32)
    weight = draw_weight(jax.random.fold_in(streams_of[8], 71), 0)
    prior = jnp.clip(jnp.exp(math.log(4.0) - 2.0794415 * jax.random.uniform(streams_of[7], (PARAMS, SOURCES), jnp.float32) ** steps_of(streams_of[7], (PARAMS, SOURCES), ((1, 32),), -0.2, 0.2)), 0.5, 4.0)
    return dict(source_id=source_id, slot=slot, owner=owner, counts=counts, partials=partials, residual=residual, weight=weight, prior=prior)


def solve_blocks(normal, moments):
    params = len(moments)
    factor = {}
    for column in range(params):
        running = normal[column][column]
        for earlier in range(column):
            running = running - factor[column, earlier] ** 2
        pivot_value = jnp.sqrt(running)
        factor[column, column] = pivot_value
        for target in range(column + 1, params):
            current = normal[target][column]
            for earlier in range(column):
                current = current - factor[target, earlier] * factor[column, earlier]
            factor[target, column] = current / pivot_value
    forward = []
    for target in range(params):
        current = moments[target]
        for earlier in range(target):
            current = current - factor[target, earlier] * forward[earlier]
        forward.append(current / factor[target, target])
    backward = [None] * params
    for target in reversed(range(params)):
        current = forward[target]
        for later in range(target + 1, params):
            current = current - factor[later, target] * backward[later]
        backward[target] = current / factor[target, target]
    return jnp.stack(backward)

def reference(source_id, slot, owner, counts, partials, residual, weight, prior):
    params = partials.shape[0]
    position = owner[source_id]
    live_mask = (slot < counts[position]).astype(jnp.float32)
    weighted = partials * (weight * live_mask)[None, :]
    normal = [[None] * params for _ in range(params)]
    for first_idx in range(params):
        for second_idx in range(first_idx, params):
            entry = jax.ops.segment_sum(weighted[first_idx] * partials[second_idx], position, num_segments=SOURCES)
            if first_idx == second_idx:
                entry = entry + prior[first_idx]
            normal[first_idx][second_idx] = entry
            normal[second_idx][first_idx] = entry
    moments = [jax.ops.segment_sum(weighted[first_idx] * residual, position, num_segments=SOURCES) for first_idx in range(params)]
    updates = solve_blocks(normal, moments)
    fitted = lax.optimization_barrier(jnp.sum(partials * updates[:, position], axis=0))
    fresh = (residual - fitted) * live_mask
    squares = jnp.sum(weight * fresh * fresh)
    live_total = jnp.sum(live_mask)
    norm = jnp.sqrt(squares / live_total + 1e-06)
    return (updates, fresh * jnp.sqrt(weight) / norm, norm)
```

```python
import functools

import jax
import jax.numpy as jnp
from jax import lax
from jax.experimental import pallas as pl
from jax.experimental.pallas import tpu as pltpu
from jax.sharding import PartitionSpec as P

LANES = 128
SUBLANES = 8
CORES = 2
MESH = pl.DeviceIdType.MESH


def solve_rows(normal, moments):
    params = len(moments)
    factor = {}
    inverse = []
    for column in range(params):
        running = normal[column][column]
        for earlier in range(column):
            running = running - factor[column, earlier] ** 2
        inverse.append(1.0 / jnp.sqrt(running))
        for target in range(column + 1, params):
            current = normal[target][column]
            for earlier in range(column):
                current = current - factor[target, earlier] * factor[column, earlier]
            factor[target, column] = current * inverse[column]
    forward = []
    for target in range(params):
        current = moments[target]
        for earlier in range(target):
            current = current - factor[target, earlier] * forward[earlier]
        forward.append(current * inverse[target])
    backward = [None] * params
    for target in reversed(range(params)):
        current = forward[target]
        for later in range(target + 1, params):
            current = current - factor[later, target] * backward[later]
        backward[target] = current * inverse[target]
    return backward


def thirds(values):
    high = values.astype(jnp.bfloat16).astype(jnp.float32)
    rest = values - high
    middle = rest.astype(jnp.bfloat16).astype(jnp.float32)
    return jnp.concatenate([high, middle, rest - middle], axis=0).astype(jnp.bfloat16)


def gather_lanes(table, index):
    return jnp.take_along_axis(table, index, axis=1, mode="promise_in_bounds")


def kernel(
    sizes,
    source_hbm, slot_hbm, owner_hbm, counts_hbm, partials_hbm, residual_hbm, weight_hbm, prior_hbm,
    updates_ref, fresh_ref, norm_ref,
    source_ref, slot_ref, owner_ref, counts_ref, partials_ref, residual_ref, weight_ref, prior_ref,
    root_buf, cell_buf, place_buf, out_buf, in_buf, meta_buf, ends_buf, sums_buf, tables,
    load_sem, send_sem, recv_sem, meta_send_sem, meta_recv_sem, sums_send_sem, sums_recv_sem,
    table_send_sem, table_recv_sem,
):
    groups, members, width, pad_slots = sizes
    n = groups * members
    params = partials_ref.shape[0]
    words = params + 2
    items = params + 1
    depth = members // CORES
    plane = groups * CORES
    pieces = width // LANES
    low = 2 if groups % 2 == 0 else 1
    high = groups // low
    row_pairs = (
        (owner_hbm, owner_ref), (source_hbm, source_ref), (slot_hbm, slot_ref), (weight_hbm, weight_ref),
        (residual_hbm, residual_ref), (partials_hbm, partials_ref), (counts_hbm, counts_ref), (prior_hbm, prior_ref),
    )
    loads = [pltpu.make_async_copy(a, b, load_sem.at[i]) for i, (a, b) in enumerate(row_pairs)]
    for load in loads:
        load.start()
    my_group, my_member = lax.axis_index("grp"), lax.axis_index("dev")
    my_depth, my_core = my_member // CORES, my_member % CORES
    me = my_group * members + my_member
    my_seat = my_group * CORES + my_core

    def target(step):
        jump = step // CORES
        group = (my_group // low + jump // low) % high * low + (my_group % low + jump % low) % low
        return group, (my_core + step % CORES) % CORES

    def origin(step):
        jump = step // CORES
        group = (my_group // low + high - jump // low) % high * low + (my_group % low + low - jump % low) % low
        return group, (my_core + CORES - step % CORES) % CORES

    def seat_coords(seat):
        group, core = seat
        return (group, my_depth * CORES + core)

    def level_coords(level):
        return (my_group, level * CORES + my_core)

    barrier = pltpu.get_barrier_semaphore()

    def greet(step, carry):
        pl.semaphore_signal(barrier, inc=1, device_id=seat_coords(target(step)), device_id_type=MESH)
        return carry

    def greet_level(step, carry):
        pl.semaphore_signal(barrier, inc=1, device_id=level_coords((my_depth + step) % depth), device_id_type=MESH)
        return carry

    lax.fori_loop(1, depth, greet_level, 0)
    lax.fori_loop(1, plane, greet, 0)

    for load in loads:
        load.wait()

    meta_buf[my_depth] = jnp.concatenate(
        [prior_ref[...], counts_ref[...].astype(jnp.float32), jnp.zeros((SUBLANES - items, LANES), jnp.float32)], axis=0
    )
    batch = min(32, owner_ref.shape[0])

    def locate(step, carry):
        rows = pl.ds(pl.multiple_of(step * SUBLANES, SUBLANES), SUBLANES)
        source = source_ref[rows, :]
        lane, tile = source % LANES, source // LANES

        def look(group, found):
            for t in range(batch):
                row = group * batch + t
                entry = jnp.broadcast_to(owner_ref[pl.ds(row, 1), :], (SUBLANES, LANES))
                found = jnp.where(tile == row, gather_lanes(entry, lane), found)
            return found

        found = jnp.full((SUBLANES, LANES), -1, jnp.int32)
        if owner_ref.shape[0] == batch:
            found = look(0, found)
        else:
            found = lax.fori_loop(0, owner_ref.shape[0] // batch, look, found)
        place = found % LANES
        place_buf[rows, :] = place
        cell = jnp.where(found < 0, -1, place * pad_slots + slot_ref[rows, :])
        cell_buf[rows, :] = cell.astype(jnp.float32)
        root = jnp.sqrt(weight_ref[rows, :])
        root_buf[rows, :] = root
        residual_ref[rows, :] = residual_ref[rows, :] * root
        return carry

    lax.fori_loop(0, source_ref.shape[0] // SUBLANES, locate, 0)

    sublane = lax.broadcasted_iota(jnp.int32, (SUBLANES, LANES), 0)

    def prepare(k, carry):
        for piece in range(pieces):
            row = pl.ds(k * pieces + piece, 1)
            cols = pl.ds(pl.multiple_of(k * width + piece * LANES, LANES), LANES)

            def spread(ref):
                return jnp.broadcast_to(ref[row, :], (SUBLANES, LANES))

            scaled = partials_ref[:, cols] * jnp.broadcast_to(root_buf[row, :], (params, LANES))
            part = slice(piece * LANES, (piece + 1) * LANES)
            out_buf[k, 0:params, part] = scaled
            out_buf[k, params:items, part] = residual_ref[row, :]
            out_buf[k, items:words, part] = cell_buf[row, :]
            out_buf[k, words : words + 1, part] = slot_ref[row, :].astype(jnp.float32)
        return carry

    lax.fori_loop(0, n, prepare, 0)

    pl.semaphore_wait(barrier, plane - 1 + depth - 1)

    def meta_copy(level, slot):
        return pltpu.make_async_remote_copy(
            src_ref=meta_buf.at[slot], dst_ref=meta_buf.at[slot], send_sem=meta_send_sem, recv_sem=meta_recv_sem,
            device_id=level_coords(level), device_id_type=MESH,
        )

    def row_copy(level, seat, slot):
        group, core = seat
        return pltpu.make_async_remote_copy(
            src_ref=out_buf.at[group * members + level * CORES + core, pl.ds(0, words)],
            dst_ref=in_buf.at[level, slot, pl.ds(0, words)],
            send_sem=send_sem, recv_sem=recv_sem.at[level, slot],
            device_id=seat_coords(seat), device_id_type=MESH,
        )

    def sums_copy(level, stage, slot):
        return pltpu.make_async_remote_copy(
            src_ref=sums_buf.at[slot, stage], dst_ref=sums_buf.at[slot, stage],
            send_sem=sums_send_sem, recv_sem=sums_recv_sem.at[stage, slot],
            device_id=level_coords(level), device_id_type=MESH,
        )

    def table_copy(stage, seat, slot):
        return pltpu.make_async_remote_copy(
            src_ref=tables.at[slot], dst_ref=tables.at[slot],
            send_sem=table_send_sem, recv_sem=table_recv_sem.at[stage],
            device_id=seat_coords(seat), device_id_type=MESH,
        )

    def send_meta(step, carry):
        meta_copy((my_depth + step) % depth, my_depth).start()
        return carry

    lax.fori_loop(1, depth, send_meta, 0)

    def send_rows(level, carry):
        def send_one(step, carry):
            row_copy(level, target(plane - 1 - step), my_seat).start()
            return carry

        return lax.fori_loop(0, plane - 1, send_one, carry)

    lax.fori_loop(0, depth, send_rows, 0)

    def own_rows(level, carry):
        in_buf[level, my_seat] = out_buf[my_group * members + level * CORES + my_core]
        return carry

    lax.fori_loop(0, depth, own_rows, 0)

    others = pl.ds(0, depth - 1)
    pltpu.make_async_remote_copy(
        src_ref=meta_buf.at[others], dst_ref=meta_buf.at[others], send_sem=meta_send_sem, recv_sem=meta_recv_sem,
        device_id=level_coords((my_depth + 1) % depth), device_id_type=MESH,
    ).wait_recv()

    src_local = counts_ref.shape[1]
    square = (src_local, LANES)
    first_cell = lax.broadcasted_iota(jnp.int32, square, 0) * pad_slots
    diagonal = lax.broadcasted_iota(jnp.int32, square, 0) == lax.broadcasted_iota(jnp.int32, square, 1)
    first_cell = first_cell.astype(jnp.float32)

    def find_ends(level, carry):
        counts = meta_buf[level, params:items, :]
        column = jnp.sum(jnp.where(diagonal, counts, 0.0), axis=1, keepdims=True)
        ends_buf[level] = first_cell + column
        return carry

    lax.fori_loop(0, depth, find_ends, 0)
    wide_sublane = lax.broadcasted_iota(jnp.int32, (SUBLANES, width), 0)

    def absorb(level, slot):
        rows = in_buf[level, slot]
        cell = rows[items:words, :]
        rows = jnp.where(wide_sublane < items, rows, 0.0)
        end_cell = ends_buf[level]
        hot = []
        for piece in range(pieces):
            part = cell[:, piece * LANES : (piece + 1) * LANES]
            hit = jnp.logical_and(part >= first_cell, part < end_cell)
            hot.append(jnp.where(hit, 1.0, 0.0))
        hot = jnp.concatenate(hot, axis=1).astype(jnp.bfloat16)
        products = jnp.concatenate([rows[i : i + 1, :] * rows for i in range(items)], axis=0)
        return lax.dot_general(
            thirds(products), hot, (((1,), (1,)), ((), ())), preferred_element_type=jnp.float32
        )

    height = items * SUBLANES

    def gather_level(level, carry):
        total = absorb(level, my_seat)

        def arrive(step, total):
            group, core = origin(plane - 1 - step)
            seat = (group, core)
            slot = group * CORES + core
            row_copy(level, seat, slot).wait_recv()
            return total + absorb(level, slot)

        total = lax.fori_loop(0, plane - 1, arrive, total)
        total = total[0:height] + total[height : 2 * height] + total[2 * height : 3 * height]
        blocks = [total[i * SUBLANES : (i + 1) * SUBLANES] for i in range(items)]
        first = jnp.where(sublane == items, pltpu.roll(blocks[5], 1, 0), blocks[0])
        second = jnp.where(
            jnp.logical_or(sublane == 0, sublane >= items), pltpu.roll(blocks[3], 3, 0), blocks[1]
        )
        third = jnp.where(sublane < 2, pltpu.roll(blocks[4], 4, 0), blocks[2])
        sums_buf[my_depth, level] = jnp.concatenate([first, second, third], axis=0)

        def send_sums(step, carry):
            sums_copy((my_depth + step) % depth, level, my_depth).start()
            return carry

        lax.fori_loop(1, depth, send_sums, 0)
        return carry

    lax.fori_loop(0, depth, gather_level, 0)

    at = {(0, 0): 0, (0, 1): 1, (0, 2): 2, (0, 3): 3, (0, 4): 4, (0, 5): 5, (5, 5): 6,
          (3, 5): 8, (1, 1): 9, (1, 2): 10, (1, 3): 11, (1, 4): 12, (1, 5): 13, (3, 3): 14, (3, 4): 15,
          (4, 4): 16, (4, 5): 17, (2, 2): 18, (2, 3): 19, (2, 4): 20, (2, 5): 21}

    def fit_level(level, carry):
        def fetch(step, carry):
            other = (my_depth + depth - step) % depth
            sums_copy(other, level, other).wait_recv()
            return carry

        lax.fori_loop(1, depth, fetch, 0)

        def gather_sums(slot, total):
            return total + sums_buf[slot, level]

        total = lax.fori_loop(1, depth, gather_sums, sums_buf[0, level])

        def entry(i, j):
            spot = at[min(i, j), max(i, j)]
            return total[spot : spot + 1, :]

        normal = [[entry(i, j) for j in range(params)] for i in range(params)]
        moments = [entry(i, params) for i in range(params)]
        with_prior = [[normal[i][j] for j in range(params)] for i in range(params)]
        for i in range(params):
            with_prior[i][i] = normal[i][i] + meta_buf[level, i : i + 1, :]
        updates = solve_rows(with_prior, moments)
        squares = entry(params, params)
        for i in range(params):
            fitted = normal[i][0] * updates[0]
            for j in range(1, params):
                fitted = fitted + normal[i][j] * updates[j]
            squares = squares + updates[i] * (fitted - 2.0 * moments[i])
        counts = meta_buf[level, params:items, :]
        mine = my_group * members + level * CORES + my_core
        tables[mine] = jnp.concatenate(updates + [jnp.full((1, LANES), -1.0, jnp.float32), squares, counts], axis=0)

        def send_table(step, carry):
            table_copy(level, target(plane - 1 - step), mine).start()
            return carry

        lax.fori_loop(0, plane - 1, send_table, 0)
        return carry

    lax.fori_loop(0, depth, fit_level, 0)
    updates_ref[...] = tables[me, 0:params, :]

    def refit_level(level, carry):
        seats = pl.ds(0, plane - 1)
        pltpu.make_async_remote_copy(
            src_ref=tables.at[seats], dst_ref=tables.at[seats],
            send_sem=table_send_sem, recv_sem=table_recv_sem.at[level],
            device_id=seat_coords(target(1)), device_id_type=MESH,
        ).wait_recv()

        def refit(seat, carry):
            k = seat // CORES * members + level * CORES + seat % CORES
            table = tables[k]
            for piece in range(pieces):
                row = pl.ds(k * pieces + piece, 1)
                place = jnp.broadcast_to(place_buf[row, :], (SUBLANES, LANES))
                picked = gather_lanes(table, place)
                rows = out_buf[k, :, piece * LANES : (piece + 1) * LANES]
                fresh = -jnp.sum(jnp.where(sublane < items, picked * rows, 0.0), axis=0, keepdims=True)
                live = rows[words : words + 1, :] < picked[words : words + 1, :]
                root_buf[row, :] = jnp.where(live, fresh, 0.0)
            return carry

        return lax.fori_loop(0, plane, refit, carry)

    lax.fori_loop(0, depth, refit_level, 0)

    def tally(k, tails):
        return tails + tables[k, items : words + 1, :]

    tails = lax.fori_loop(0, n, tally, jnp.zeros((2, LANES), jnp.float32))
    tails = jnp.sum(tails, axis=1, keepdims=True)
    norm = jnp.sqrt(jnp.maximum(tails[0:1], 0.0) / tails[1:2] + 1e-06)
    norm_ref[...] = jnp.broadcast_to(norm, norm_ref.shape)
    scale = 1.0 / norm
    fresh_ref[...] = root_buf[...] * scale

    def drain(ref, semaphore):
        pltpu.make_async_remote_copy(
            src_ref=ref, dst_ref=ref, send_sem=semaphore, recv_sem=meta_recv_sem,
            device_id=seat_coords(target(1)), device_id_type=MESH,
        ).wait_send()

    sent = depth * (plane - 1)
    drain(out_buf.at[pl.ds(0, sent), pl.ds(0, words)], send_sem)
    drain(meta_buf.at[others], meta_send_sem)
    drain(sums_buf.at[others], sums_send_sem)
    drain(tables.at[pl.ds(0, sent)], table_send_sem)


def release(a_ref, b_ref, c_ref, a_out, b_out, c_out, sem):
    pairs = ((a_ref, a_out), (b_ref, b_out), (c_ref, c_out))
    copies = [pltpu.make_async_copy(x, y, sem.at[i]) for i, (x, y) in enumerate(pairs)]
    for copy in copies:
        copy.start()
    for copy in copies:
        copy.wait()


def body(source_id, slot, owner, counts, partials, residual, weight, prior):
    groups, members = lax.axis_size("grp"), lax.axis_size("dev")
    n = groups * members
    params = partials.shape[0]
    row_count = residual.shape[0]
    src_local = counts.shape[0]
    block_rows = row_count // n
    width = -(-block_rows // LANES) * LANES
    depth, plane = members // CORES, groups * CORES

    def lay(array, fill):
        if width == block_rows:
            return array
        blocks = array.reshape(-1, n, block_rows)
        blocks = jnp.pad(blocks, ((0, 0), (0, 0), (0, width - block_rows)), constant_values=fill)
        return blocks.reshape(array.shape[:-1] + (n * width,))

    def dense(array, fill):
        return lay(array, fill).reshape(-1, LANES)

    vmem = pl.BlockSpec(memory_space=pltpu.VMEM)
    operands = (
        dense(source_id, -1),
        dense(slot, 0),
        owner.reshape(-1, LANES),
        counts.reshape(1, src_local),
        lay(partials, 0),
        dense(residual, 0),
        dense(weight, 1),
        prior,
    )
    rows = n * width // LANES
    updates, standardized, norm = pl.pallas_call(
        functools.partial(kernel, (groups, members, width, row_count // src_local)),
        out_shape=(
            jax.ShapeDtypeStruct((params, src_local), jnp.float32),
            jax.ShapeDtypeStruct((rows, LANES), jnp.float32),
            jax.ShapeDtypeStruct((1, LANES), jnp.float32),
        ),
        in_specs=[pl.BlockSpec(memory_space=pltpu.HBM)] * len(operands),
        out_specs=(vmem, vmem, vmem),
        scratch_shapes=[pltpu.VMEM(operand.shape, operand.dtype) for operand in operands] + [
            pltpu.VMEM((rows, LANES), jnp.float32),
            pltpu.VMEM((rows, LANES), jnp.float32),
            pltpu.VMEM((rows, LANES), jnp.int32),
            pltpu.VMEM((n, SUBLANES, width), jnp.float32),
            pltpu.VMEM((depth, plane, SUBLANES, width), jnp.float32),
            pltpu.VMEM((depth, SUBLANES, LANES), jnp.float32),
            pltpu.VMEM((depth, src_local, LANES), jnp.float32),
            pltpu.VMEM((depth, depth, 3 * SUBLANES, LANES), jnp.float32),
            pltpu.VMEM((n, SUBLANES, LANES), jnp.float32),
            pltpu.SemaphoreType.DMA((len(operands),)),
            pltpu.SemaphoreType.DMA,
            pltpu.SemaphoreType.DMA((depth, plane)),
            pltpu.SemaphoreType.DMA,
            pltpu.SemaphoreType.DMA,
            pltpu.SemaphoreType.DMA,
            pltpu.SemaphoreType.DMA((depth, depth)),
            pltpu.SemaphoreType.DMA,
            pltpu.SemaphoreType.DMA((depth,)),
        ],
        compiler_params=pltpu.CompilerParams(
            collective_id=0, has_side_effects=True, vmem_limit_bytes=65000 * 1024
        ),
        name="exchange_fit",
    )(*operands)
    results = (updates, standardized, norm)
    updates, standardized, norm = pl.pallas_call(
        release,
        out_shape=tuple(jax.ShapeDtypeStruct(r.shape, r.dtype) for r in results),
        in_specs=[vmem] * 3,
        out_specs=[pl.BlockSpec(memory_space=pltpu.HBM)] * 3,
        scratch_shapes=[pltpu.SemaphoreType.DMA((3,))],
        name="release",
    )(*results)
    standardized = standardized.reshape(n, width)[:, :block_rows] if width != block_rows else standardized
    return (updates, standardized.reshape(row_count), norm[0, 0])


def solution(mesh):
    in_specs = (
        P(("grp", "dev")),
        P(("grp", "dev")),
        P(),
        P(("grp", "dev")),
        P(None, ("grp", "dev")),
        P(("grp", "dev")),
        P(("grp", "dev")),
        P(None, ("grp", "dev")),
    )
    out_specs = (P(None, ("grp", "dev")), P(("grp", "dev")), P())
    return jax.shard_map(body, mesh=mesh, in_specs=in_specs, out_specs=out_specs, check_vma=False)
```

```python
import functools

import jax
import jax.numpy as jnp
from jax import lax
from jax.experimental import pallas as pl
from jax.experimental.pallas import tpu as pltpu
from jax.sharding import PartitionSpec as P

LANES = 128
SUBLANES = 8
CORES = 2
MESH = pl.DeviceIdType.MESH


def solve_rows(normal, moments):
    params = len(moments)
    factor = {}
    inverse = []
    for column in range(params):
        running = normal[column][column]
        for earlier in range(column):
            running = running - factor[column, earlier] ** 2
        inverse.append(1.0 / jnp.sqrt(running))
        for target in range(column + 1, params):
            current = normal[target][column]
            for earlier in range(column):
                current = current - factor[target, earlier] * factor[column, earlier]
            factor[target, column] = current * inverse[column]
    forward = []
    for target in range(params):
        current = moments[target]
        for earlier in range(target):
            current = current - factor[target, earlier] * forward[earlier]
        forward.append(current * inverse[target])
    backward = [None] * params
    for target in reversed(range(params)):
        current = forward[target]
        for later in range(target + 1, params):
            current = current - factor[later, target] * backward[later]
        backward[target] = current * inverse[target]
    return backward


def thirds(values):
    high = values.astype(jnp.bfloat16).astype(jnp.float32)
    rest = values - high
    middle = rest.astype(jnp.bfloat16).astype(jnp.float32)
    return jnp.concatenate([high, middle, rest - middle], axis=0).astype(jnp.bfloat16)


def gather_lanes(table, index):
    return jnp.take_along_axis(table, index, axis=1, mode="promise_in_bounds")


def kernel(
    sizes,
    source_hbm, slot_hbm, owner_hbm, counts_hbm, partials_hbm, residual_hbm, weight_hbm, prior_hbm,
    updates_ref, fresh_ref, norm_ref,
    source_ref, slot_ref, owner_ref, counts_ref, partials_ref, residual_ref, weight_ref, prior_ref,
    root_buf, cell_buf, place_buf, out_buf, in_buf, meta_buf, first_buf, ends_buf, sums_buf, tables,
    load_sem, send_sem, recv_sem, meta_send_sem, meta_recv_sem, sums_send_sem, sums_recv_sem,
    table_send_sem, table_recv_sem,
):
    groups, members, width, pad_slots = sizes
    n = groups * members
    params = partials_ref.shape[0]
    words = params + 2
    items = params + 1
    depth = members // CORES
    plane = groups * CORES
    pieces = width // LANES
    low = 2 if groups % 2 == 0 else 1
    high = groups // low
    row_pairs = (
        (owner_hbm, owner_ref), (source_hbm, source_ref), (slot_hbm, slot_ref), (weight_hbm, weight_ref),
        (residual_hbm, residual_ref), (partials_hbm, partials_ref), (counts_hbm, counts_ref), (prior_hbm, prior_ref),
    )
    loads = [pltpu.make_async_copy(a, b, load_sem.at[i]) for i, (a, b) in enumerate(row_pairs)]
    for load in loads:
        load.start()
    my_group, my_member = lax.axis_index("grp"), lax.axis_index("dev")
    my_depth, my_core = my_member // CORES, my_member % CORES
    me = my_group * members + my_member
    my_seat = my_group * CORES + my_core

    def target(step):
        jump = step // CORES
        group = (my_group // low + jump // low) % high * low + (my_group % low + jump % low) % low
        return group, (my_core + step % CORES) % CORES

    def origin(step):
        jump = step // CORES
        group = (my_group // low + high - jump // low) % high * low + (my_group % low + low - jump % low) % low
        return group, (my_core + CORES - step % CORES) % CORES

    def seat_coords(seat):
        group, core = seat
        return (group, my_depth * CORES + core)

    def level_coords(level):
        return (my_group, level * CORES + my_core)

    barrier = pltpu.get_barrier_semaphore()

    def greet(step, carry):
        pl.semaphore_signal(barrier, inc=1, device_id=seat_coords(target(step)), device_id_type=MESH)
        return carry

    def greet_level(step, carry):
        pl.semaphore_signal(barrier, inc=1, device_id=level_coords((my_depth + step) % depth), device_id_type=MESH)
        return carry

    lax.fori_loop(1, depth, greet_level, 0)
    lax.fori_loop(1, plane, greet, 0)

    for load in loads:
        load.wait()

    root = jnp.sqrt(weight_ref[...])
    root_buf[...] = root
    residual_ref[...] = residual_ref[...] * root
    cell_buf[...] = (source_ref[...] * pad_slots + slot_ref[...]).astype(jnp.float32)

    sublane = lax.broadcasted_iota(jnp.int32, (SUBLANES, LANES), 0)

    def prepare(k, carry):
        for piece in range(pieces):
            row = pl.ds(k * pieces + piece, 1)
            cols = pl.ds(pl.multiple_of(k * width + piece * LANES, LANES), LANES)

            def spread(ref):
                return jnp.broadcast_to(ref[row, :], (SUBLANES, LANES))

            scaled = partials_ref[:, cols] * jnp.broadcast_to(root_buf[row, :], (params, LANES))
            part = slice(piece * LANES, (piece + 1) * LANES)
            out_buf[k, 0:params, part] = scaled
            out_buf[k, params:items, part] = residual_ref[row, :]
            out_buf[k, items:words, part] = cell_buf[row, :]
            out_buf[k, words : words + 1, part] = slot_ref[row, :].astype(jnp.float32)
        return carry

    lax.fori_loop(0, n, prepare, 0)

    src_local = counts_ref.shape[1]
    square = (src_local, LANES)
    row_index = lax.broadcasted_iota(jnp.int32, square, 0)
    lane_index = lax.broadcasted_iota(jnp.int32, square, 1)
    diagonal = row_index == lane_index

    def invert(tile, total):
        ids = tile * LANES + lax.broadcasted_iota(jnp.int32, (1, LANES), 1)
        return total + jnp.where(owner_ref[pl.ds(tile, 1), :] == row_index + me * src_local, ids, 0)

    found = lax.fori_loop(0, owner_ref.shape[0], invert, jnp.zeros(square, jnp.int32))
    source_at = jnp.sum(found.astype(jnp.float32), axis=1, keepdims=True)
    source_at = jnp.sum(jnp.where(diagonal, source_at, 0.0), axis=0, keepdims=True)
    meta_buf[my_depth] = jnp.concatenate(
        [prior_ref[...], counts_ref[...].astype(jnp.float32), source_at * pad_slots]
        + [jnp.zeros((SUBLANES - words, LANES), jnp.float32)],
        axis=0,
    )

    pl.semaphore_wait(barrier, plane - 1 + depth - 1)

    def meta_copy(level, slot):
        return pltpu.make_async_remote_copy(
            src_ref=meta_buf.at[slot], dst_ref=meta_buf.at[slot], send_sem=meta_send_sem, recv_sem=meta_recv_sem,
            device_id=level_coords(level), device_id_type=MESH,
        )

    def row_copy(level, seat, slot):
        group, core = seat
        return pltpu.make_async_remote_copy(
            src_ref=out_buf.at[group * members + level * CORES + core, pl.ds(0, words)],
            dst_ref=in_buf.at[level, slot, pl.ds(0, words)],
            send_sem=send_sem, recv_sem=recv_sem.at[level, slot],
            device_id=seat_coords(seat), device_id_type=MESH,
        )

    def sums_copy(level, stage, slot):
        return pltpu.make_async_remote_copy(
            src_ref=sums_buf.at[slot, stage], dst_ref=sums_buf.at[slot, stage],
            send_sem=sums_send_sem, recv_sem=sums_recv_sem.at[stage, slot],
            device_id=level_coords(level), device_id_type=MESH,
        )

    def table_copy(stage, seat, slot):
        return pltpu.make_async_remote_copy(
            src_ref=tables.at[slot], dst_ref=tables.at[slot],
            send_sem=table_send_sem, recv_sem=table_recv_sem.at[stage],
            device_id=seat_coords(seat), device_id_type=MESH,
        )

    def send_meta(step, carry):
        meta_copy((my_depth + step) % depth, my_depth).start()
        return carry

    lax.fori_loop(1, depth, send_meta, 0)

    def send_rows(level, carry):
        def send_one(step, carry):
            row_copy(level, target(plane - 1 - step), my_seat).start()
            return carry

        return lax.fori_loop(0, plane - 1, send_one, carry)

    lax.fori_loop(0, depth, send_rows, 0)

    def own_rows(level, carry):
        in_buf[level, my_seat] = out_buf[my_group * members + level * CORES + my_core]
        return carry

    lax.fori_loop(0, depth, own_rows, 0)

    others = pl.ds(0, depth - 1)
    pltpu.make_async_remote_copy(
        src_ref=meta_buf.at[others], dst_ref=meta_buf.at[others], send_sem=meta_send_sem, recv_sem=meta_recv_sem,
        device_id=level_coords((my_depth + 1) % depth), device_id_type=MESH,
    ).wait_recv()

    def find_cells(level, carry):
        first = jnp.sum(jnp.where(diagonal, meta_buf[level, items:words, :], 0.0), axis=1, keepdims=True)
        counts = jnp.sum(jnp.where(diagonal, meta_buf[level, params:items, :], 0.0), axis=1, keepdims=True)
        first_buf[level] = jnp.broadcast_to(first, square)
        ends_buf[level] = jnp.broadcast_to(first + counts, square)
        return carry

    lax.fori_loop(0, depth, find_cells, 0)
    wide_sublane = lax.broadcasted_iota(jnp.int32, (SUBLANES, width), 0)

    def absorb(level, slots):
        first_cell, end_cell = first_buf[level], ends_buf[level]
        hot, products = [], []
        for slot in slots:
            rows = in_buf[level, slot]
            cell = rows[items:words, :]
            rows = jnp.where(wide_sublane < items, rows, 0.0)
            for piece in range(pieces):
                part = cell[:, piece * LANES : (piece + 1) * LANES]
                hit = jnp.logical_and(part >= first_cell, part < end_cell)
                hot.append(jnp.where(hit, 1.0, 0.0))
            products.append(jnp.concatenate([rows[i : i + 1, :] * rows for i in range(items)], axis=0))
        hot = jnp.concatenate(hot, axis=1).astype(jnp.bfloat16)
        products = jnp.concatenate(products, axis=1)
        return lax.dot_general(
            thirds(products), hot, (((1,), (1,)), ((), ())), preferred_element_type=jnp.float32
        )

    height = items * SUBLANES

    def gather_level(level, carry):
        def arrive(steps):
            slots = []
            for step in steps:
                group, core = origin(step)
                slot = group * CORES + core
                if step:
                    row_copy(level, (group, core), slot).wait_recv()
                slots.append(slot)
            return absorb(level, slots)

        half = plane // 2
        total = arrive([0] + list(range(plane - 1, half, -1))) + arrive(range(half, 0, -1))
        total = total[0:height] + total[height : 2 * height] + total[2 * height : 3 * height]
        blocks = [total[i * SUBLANES : (i + 1) * SUBLANES] for i in range(items)]
        first = jnp.where(sublane == items, pltpu.roll(blocks[5], 1, 0), blocks[0])
        second = jnp.where(
            jnp.logical_or(sublane == 0, sublane >= items), pltpu.roll(blocks[3], 3, 0), blocks[1]
        )
        third = jnp.where(sublane < 2, pltpu.roll(blocks[4], 4, 0), blocks[2])
        sums_buf[my_depth, level] = jnp.concatenate([first, second, third], axis=0)

        def send_sums(step, carry):
            sums_copy((my_depth + step) % depth, level, my_depth).start()
            return carry

        lax.fori_loop(1, depth, send_sums, 0)
        return carry

    lax.fori_loop(0, depth, gather_level, 0)
    batch = min(32, owner_ref.shape[0])

    def locate(step, carry):
        rows = pl.ds(pl.multiple_of(step * SUBLANES, SUBLANES), SUBLANES)
        source = source_ref[rows, :]
        lane, tile = source % LANES, source // LANES

        def look(group, found):
            for t in range(batch):
                row = group * batch + t
                entry = jnp.broadcast_to(owner_ref[pl.ds(row, 1), :], (SUBLANES, LANES))
                found = jnp.where(tile == row, gather_lanes(entry, lane), found)
            return found

        found = jnp.full((SUBLANES, LANES), -1, jnp.int32)
        if owner_ref.shape[0] == batch:
            found = look(0, found)
        else:
            found = lax.fori_loop(0, owner_ref.shape[0] // batch, look, found)
        place_buf[rows, :] = found % LANES
        return carry

    lax.fori_loop(0, source_ref.shape[0] // SUBLANES, locate, 0)


    at = {(0, 0): 0, (0, 1): 1, (0, 2): 2, (0, 3): 3, (0, 4): 4, (0, 5): 5, (5, 5): 6,
          (3, 5): 8, (1, 1): 9, (1, 2): 10, (1, 3): 11, (1, 4): 12, (1, 5): 13, (3, 3): 14, (3, 4): 15,
          (4, 4): 16, (4, 5): 17, (2, 2): 18, (2, 3): 19, (2, 4): 20, (2, 5): 21}

    def fit_level(level, carry):
        def fetch(step, carry):
            other = (my_depth + depth - step) % depth
            sums_copy(other, level, other).wait_recv()
            return carry

        lax.fori_loop(1, depth, fetch, 0)

        def gather_sums(slot, total):
            return total + sums_buf[slot, level]

        total = lax.fori_loop(1, depth, gather_sums, sums_buf[0, level])

        def entry(i, j):
            spot = at[min(i, j), max(i, j)]
            return total[spot : spot + 1, :]

        normal = [[entry(i, j) for j in range(params)] for i in range(params)]
        moments = [entry(i, params) for i in range(params)]
        with_prior = [[normal[i][j] for j in range(params)] for i in range(params)]
        for i in range(params):
            with_prior[i][i] = normal[i][i] + meta_buf[level, i : i + 1, :]
        updates = solve_rows(with_prior, moments)
        squares = entry(params, params)
        for i in range(params):
            fitted = normal[i][0] * updates[0]
            for j in range(1, params):
                fitted = fitted + normal[i][j] * updates[j]
            squares = squares + updates[i] * (fitted - 2.0 * moments[i])
        counts = meta_buf[level, params:items, :]
        mine = my_group * members + level * CORES + my_core
        tables[mine] = jnp.concatenate(updates + [jnp.full((1, LANES), -1.0, jnp.float32), squares, counts], axis=0)

        def send_table(step, carry):
            table_copy(level, target(plane - 1 - step), mine).start()
            return carry

        lax.fori_loop(0, plane - 1, send_table, 0)
        return carry

    lax.fori_loop(0, depth, fit_level, 0)
    updates_ref[...] = tables[me, 0:params, :]

    def refit_level(level, tails):
        seats = pl.ds(0, plane - 1)
        pltpu.make_async_remote_copy(
            src_ref=tables.at[seats], dst_ref=tables.at[seats],
            send_sem=table_send_sem, recv_sem=table_recv_sem.at[level],
            device_id=seat_coords(target(1)), device_id_type=MESH,
        ).wait_recv()

        for seat in range(plane):
            k = seat // CORES * members + level * CORES + seat % CORES
            table = tables[k]
            tails = tails + table[items : words + 1, :]
            for piece in range(pieces):
                row = pl.ds(k * pieces + piece, 1)
                place = jnp.broadcast_to(place_buf[row, :], (SUBLANES, LANES))
                picked = gather_lanes(table, place)
                rows = out_buf[k, :, piece * LANES : (piece + 1) * LANES]
                fresh = -jnp.sum(jnp.where(sublane < items, picked * rows, 0.0), axis=0, keepdims=True)
                live = rows[words : words + 1, :] < picked[words : words + 1, :]
                root_buf[row, :] = jnp.where(live, fresh, 0.0)
        return tails

    tails = lax.fori_loop(0, depth, refit_level, jnp.zeros((2, LANES), jnp.float32))
    tails = jnp.sum(tails, axis=1, keepdims=True)
    norm = jnp.sqrt(jnp.maximum(tails[0:1], 0.0) / tails[1:2] + 1e-06)
    norm_ref[...] = jnp.broadcast_to(norm, norm_ref.shape)
    scale = 1.0 / norm
    fresh_ref[...] = root_buf[...] * scale

    def drain(ref, semaphore):
        pltpu.make_async_remote_copy(
            src_ref=ref, dst_ref=ref, send_sem=semaphore, recv_sem=meta_recv_sem,
            device_id=seat_coords(target(1)), device_id_type=MESH,
        ).wait_send()

    sent = depth * (plane - 1)
    drain(out_buf.at[pl.ds(0, sent), pl.ds(0, words)], send_sem)
    drain(meta_buf.at[others], meta_send_sem)
    drain(sums_buf.at[others], sums_send_sem)
    drain(tables.at[pl.ds(0, sent)], table_send_sem)


def release(a_ref, b_ref, c_ref, a_out, b_out, c_out, sem):
    pairs = ((a_ref, a_out), (b_ref, b_out), (c_ref, c_out))
    copies = [pltpu.make_async_copy(x, y, sem.at[i]) for i, (x, y) in enumerate(pairs)]
    for copy in copies:
        copy.start()
    for copy in copies:
        copy.wait()


def body(source_id, slot, owner, counts, partials, residual, weight, prior):
    groups, members = lax.axis_size("grp"), lax.axis_size("dev")
    n = groups * members
    params = partials.shape[0]
    row_count = residual.shape[0]
    src_local = counts.shape[0]
    block_rows = row_count // n
    width = -(-block_rows // LANES) * LANES
    depth, plane = members // CORES, groups * CORES

    def lay(array, fill):
        if width == block_rows:
            return array
        blocks = array.reshape(-1, n, block_rows)
        blocks = jnp.pad(blocks, ((0, 0), (0, 0), (0, width - block_rows)), constant_values=fill)
        return blocks.reshape(array.shape[:-1] + (n * width,))

    def dense(array, fill):
        return lay(array, fill).reshape(-1, LANES)

    vmem = pl.BlockSpec(memory_space=pltpu.VMEM)
    operands = (
        dense(source_id, -1),
        dense(slot, 0),
        owner.reshape(-1, LANES),
        counts.reshape(1, src_local),
        lay(partials, 0),
        dense(residual, 0),
        dense(weight, 1),
        prior,
    )
    operands = tuple(pltpu.with_memory_space_constraint(x, pltpu.HBM) for x in operands)
    rows = n * width // LANES
    updates, standardized, norm = pl.pallas_call(
        functools.partial(kernel, (groups, members, width, row_count // src_local)),
        out_shape=(
            pltpu.VMEM((params, src_local), jnp.float32),
            pltpu.VMEM((rows, LANES), jnp.float32),
            pltpu.VMEM((1, LANES), jnp.float32),
        ),
        in_specs=[pl.BlockSpec(memory_space=pltpu.HBM)] * len(operands),
        out_specs=(vmem, vmem, vmem),
        scratch_shapes=[pltpu.VMEM(operand.shape, operand.dtype) for operand in operands] + [
            pltpu.VMEM((rows, LANES), jnp.float32),
            pltpu.VMEM((rows, LANES), jnp.float32),
            pltpu.VMEM((rows, LANES), jnp.int32),
            pltpu.VMEM((n, SUBLANES, width), jnp.float32),
            pltpu.VMEM((depth, plane, SUBLANES, width), jnp.float32),
            pltpu.VMEM((depth, SUBLANES, LANES), jnp.float32),
            pltpu.VMEM((depth, src_local, LANES), jnp.float32),
            pltpu.VMEM((depth, src_local, LANES), jnp.float32),
            pltpu.VMEM((depth, depth, 3 * SUBLANES, LANES), jnp.float32),
            pltpu.VMEM((n, SUBLANES, LANES), jnp.float32),
            pltpu.SemaphoreType.DMA((len(operands),)),
            pltpu.SemaphoreType.DMA,
            pltpu.SemaphoreType.DMA((depth, plane)),
            pltpu.SemaphoreType.DMA,
            pltpu.SemaphoreType.DMA,
            pltpu.SemaphoreType.DMA,
            pltpu.SemaphoreType.DMA((depth, depth)),
            pltpu.SemaphoreType.DMA,
            pltpu.SemaphoreType.DMA((depth,)),
        ],
        compiler_params=pltpu.CompilerParams(
            collective_id=0, has_side_effects=True, vmem_limit_bytes=40 << 20
        ),
        name="exchange_fit",
    )(*operands)
    results = (updates, standardized, norm)
    updates, standardized, norm = pl.pallas_call(
        release,
        out_shape=tuple(jax.ShapeDtypeStruct(r.shape, r.dtype) for r in results),
        in_specs=[vmem] * 3,
        out_specs=[pl.BlockSpec(memory_space=pltpu.HBM)] * 3,
        scratch_shapes=[pltpu.SemaphoreType.DMA((3,))],
        compiler_params=pltpu.CompilerParams(vmem_limit_bytes=4 << 20),
        name="release",
    )(*results)
    standardized = standardized.reshape(n, width)[:, :block_rows] if width != block_rows else standardized
    return (updates, standardized.reshape(row_count), norm[0, 0])


def solution(mesh):
    in_specs = (
        P(("grp", "dev")),
        P(("grp", "dev")),
        P(),
        P(("grp", "dev")),
        P(None, ("grp", "dev")),
        P(("grp", "dev")),
        P(("grp", "dev")),
        P(None, ("grp", "dev")),
    )
    out_specs = (P(None, ("grp", "dev")), P(("grp", "dev")), P())
    return jax.shard_map(body, mesh=mesh, in_specs=in_specs, out_specs=out_specs, check_vma=False)
```

```python
import functools

import jax
import jax.numpy as jnp
from jax import lax
from jax.experimental import pallas as pl
from jax.experimental.pallas import tpu as pltpu
from jax.sharding import PartitionSpec as P

LANES = 128
SUBLANES = 8
CORES = 2
MESH = pl.DeviceIdType.MESH


def solve_rows(normal, moments):
    params = len(moments)
    factor = {}
    inverse = []
    for column in range(params):
        running = normal[column][column]
        for earlier in range(column):
            running = running - factor[column, earlier] ** 2
        inverse.append(1.0 / jnp.sqrt(running))
        for target in range(column + 1, params):
            current = normal[target][column]
            for earlier in range(column):
                current = current - factor[target, earlier] * factor[column, earlier]
            factor[target, column] = current * inverse[column]
    forward = []
    for target in range(params):
        current = moments[target]
        for earlier in range(target):
            current = current - factor[target, earlier] * forward[earlier]
        forward.append(current * inverse[target])
    backward = [None] * params
    for target in reversed(range(params)):
        current = forward[target]
        for later in range(target + 1, params):
            current = current - factor[later, target] * backward[later]
        backward[target] = current * inverse[target]
    return backward


def thirds(values):
    high = values.astype(jnp.bfloat16)
    rest = values - high.astype(jnp.float32)
    middle = rest.astype(jnp.bfloat16)
    last = (rest - middle.astype(jnp.float32)).astype(jnp.bfloat16)
    return jnp.concatenate([high, middle, last], axis=0)


def gather_lanes(table, index):
    return jnp.take_along_axis(table, index, axis=1, mode="promise_in_bounds")


def kernel(
    sizes,
    source_hbm, slot_hbm, owner_hbm, counts_hbm, partials_hbm, residual_hbm, weight_hbm, prior_hbm,
    updates_ref, fresh_ref, norm_ref,
    source_ref, slot_ref, owner_ref, counts_ref, partials_ref, residual_ref, weight_ref, prior_ref,
    root_buf, cell_buf, place_buf, out_buf, in_buf, meta_buf, first_buf, room_buf, sums_buf, tables,
    load_sem, send_sem, recv_sem, meta_send_sem, meta_recv_sem, sums_send_sem, sums_recv_sem,
    table_send_sem, table_recv_sem,
):
    groups, members, width, pad_slots = sizes
    n = groups * members
    params = partials_ref.shape[0]
    words = params + 2
    items = params + 1
    depth = members // CORES
    plane = groups * CORES
    pieces = width // LANES
    low = 2 if groups % 2 == 0 else 1
    high = groups // low
    my_group, my_member = lax.axis_index("grp"), lax.axis_index("dev")
    my_depth, my_core = my_member // CORES, my_member % CORES
    me = my_group * members + my_member
    my_seat = my_group * CORES + my_core

    def target(step):
        jump = step // CORES
        group = (my_group // low + jump // low) % high * low + (my_group % low + jump % low) % low
        return group, (my_core + step % CORES) % CORES

    def origin(step):
        jump = step // CORES
        group = (my_group // low + high - jump // low) % high * low + (my_group % low + low - jump % low) % low
        return group, (my_core + CORES - step % CORES) % CORES

    def seat_coords(seat):
        group, core = seat
        return (group, my_depth * CORES + core)

    def level_coords(level):
        return (my_group, level * CORES + my_core)

    barrier = pltpu.get_barrier_semaphore()

    def greet(step, carry):
        pl.semaphore_signal(barrier, inc=1, device_id=seat_coords(target(step)), device_id_type=MESH)
        return carry

    def greet_level(step, carry):
        pl.semaphore_signal(barrier, inc=1, device_id=level_coords((my_depth + step) % depth), device_id_type=MESH)
        return carry

    lax.fori_loop(1, depth, greet_level, 0)
    lax.fori_loop(1, plane, greet, 0)
    row_pairs = (
        (owner_hbm, owner_ref), (source_hbm, source_ref), (slot_hbm, slot_ref), (weight_hbm, weight_ref),
        (residual_hbm, residual_ref), (partials_hbm, partials_ref), (counts_hbm, counts_ref), (prior_hbm, prior_ref),
    )
    loads = [pltpu.make_async_copy(a, b, load_sem.at[i]) for i, (a, b) in enumerate(row_pairs)]
    for load in loads:
        load.start()

    for load in loads:
        load.wait()

    root = jnp.sqrt(weight_ref[...])
    root_buf[...] = root
    residual_ref[...] = residual_ref[...] * root
    cell_buf[...] = (source_ref[...] * pad_slots + slot_ref[...]).astype(jnp.float32)

    sublane = lax.broadcasted_iota(jnp.int32, (SUBLANES, LANES), 0)

    def prepare(k, carry):
        for piece in range(pieces):
            row = pl.ds(k * pieces + piece, 1)
            cols = pl.ds(pl.multiple_of(k * width + piece * LANES, LANES), LANES)

            def spread(ref):
                return jnp.broadcast_to(ref[row, :], (SUBLANES, LANES))

            scaled = partials_ref[:, cols] * jnp.broadcast_to(root_buf[row, :], (params, LANES))
            part = slice(piece * LANES, (piece + 1) * LANES)
            out_buf[k, 0:params, part] = scaled
            out_buf[k, params:items, part] = residual_ref[row, :]
            out_buf[k, items:words, part] = cell_buf[row, :]
            out_buf[k, words : words + 1, part] = slot_ref[row, :].astype(jnp.float32)
        return carry

    lax.fori_loop(0, n, prepare, 0)

    pl.semaphore_wait(barrier, plane - 1 + depth - 1)

    def meta_copy(level, slot):
        return pltpu.make_async_remote_copy(
            src_ref=meta_buf.at[slot], dst_ref=meta_buf.at[slot], send_sem=meta_send_sem, recv_sem=meta_recv_sem,
            device_id=level_coords(level), device_id_type=MESH,
        )

    def row_copy(level, seat, slot, part):
        group, core = seat
        return pltpu.make_async_remote_copy(
            src_ref=out_buf.at[group * members + level * CORES + core, pl.ds(0, words)],
            dst_ref=in_buf.at[level, slot, pl.ds(0, words)],
            send_sem=send_sem, recv_sem=recv_sem.at[level, part],
            device_id=seat_coords(seat), device_id_type=MESH,
        )

    def sums_copy(level, stage, slot):
        return pltpu.make_async_remote_copy(
            src_ref=sums_buf.at[slot, stage], dst_ref=sums_buf.at[slot, stage],
            send_sem=sums_send_sem, recv_sem=sums_recv_sem.at[stage],
            device_id=level_coords(level), device_id_type=MESH,
        )

    def table_copy(stage, seat, slot):
        return pltpu.make_async_remote_copy(
            src_ref=tables.at[slot], dst_ref=tables.at[slot],
            send_sem=table_send_sem, recv_sem=table_recv_sem.at[stage],
            device_id=seat_coords(seat), device_id_type=MESH,
        )

    half = plane // 2
    batches = ([0] + list(range(plane - 1, half, -1)), list(range(half, 0, -1)))

    def send_rows(level, carry):
        for part, steps in enumerate(batches):
            for step in steps:
                if step:
                    row_copy(level, target(step), my_seat, part).start()
        return carry

    lax.fori_loop(0, depth, send_rows, 0)

    def own_rows(level, carry):
        in_buf[level, my_seat] = out_buf[my_group * members + level * CORES + my_core]
        return carry

    lax.fori_loop(0, depth, own_rows, 0)

    src_local = counts_ref.shape[1]
    square = (src_local, LANES)
    row_index = lax.broadcasted_iota(jnp.int32, square, 0)
    lane_index = lax.broadcasted_iota(jnp.int32, square, 1)
    diagonal = row_index == lane_index

    spare = 4

    def invert(step, total):
        for part in range(spare):
            tile = step * spare + part
            ids = tile * LANES + lane_index
            total = jnp.where(owner_ref[pl.ds(tile, 1), :] == row_index + me * src_local, ids, total)
        return total

    found = lax.fori_loop(0, owner_ref.shape[0] // spare, invert, jnp.zeros(square, jnp.int32))
    source_at = jnp.sum(found.astype(jnp.float32), axis=1, keepdims=True)
    source_at = jnp.sum(jnp.where(diagonal, source_at, 0.0), axis=0, keepdims=True)
    meta_buf[my_depth] = jnp.concatenate(
        [prior_ref[...], counts_ref[...].astype(jnp.float32), source_at * pad_slots]
        + [jnp.zeros((SUBLANES - words, LANES), jnp.float32)],
        axis=0,
    )

    def send_meta(step, carry):
        meta_copy((my_depth + step) % depth, my_depth).start()
        return carry

    lax.fori_loop(1, depth, send_meta, 0)

    batch = min(32, owner_ref.shape[0])

    def locate(step, carry):
        rows = pl.ds(pl.multiple_of(step * SUBLANES, SUBLANES), SUBLANES)
        source = source_ref[rows, :]
        lane, tile = source % LANES, source // LANES

        def look(group, found):
            for t in range(batch):
                row = group * batch + t
                entry = jnp.broadcast_to(owner_ref[pl.ds(row, 1), :], (SUBLANES, LANES))
                found = jnp.where(tile == row, gather_lanes(entry, lane), found)
            return found

        found = jnp.full((SUBLANES, LANES), -1, jnp.int32)
        if owner_ref.shape[0] == batch:
            found = look(0, found)
        else:
            found = lax.fori_loop(0, owner_ref.shape[0] // batch, look, found)
        place_buf[rows, :] = found % LANES
        return carry

    lax.fori_loop(0, source_ref.shape[0] // SUBLANES, locate, 0)


    others = pl.ds(0, depth - 1)
    pltpu.make_async_remote_copy(
        src_ref=meta_buf.at[others], dst_ref=meta_buf.at[others], send_sem=meta_send_sem, recv_sem=meta_recv_sem,
        device_id=level_coords((my_depth + 1) % depth), device_id_type=MESH,
    ).wait_recv()

    def find_cells(level, carry):
        first, counts = meta_buf[level, items:words, :], meta_buf[level, params:items, :]
        first = jnp.sum(jnp.where(diagonal, first, 0.0), axis=1, keepdims=True)
        counts = jnp.sum(jnp.where(diagonal, counts, 0.0), axis=1, keepdims=True)
        first_buf[level] = jnp.broadcast_to(first, square).astype(jnp.int32)
        room_buf[level] = jnp.broadcast_to(counts, square).astype(jnp.int32).astype(jnp.uint32)
        return carry

    lax.fori_loop(0, depth, find_cells, 0, unroll=depth if depth <= 4 else 1)
    wide_sublane = lax.broadcasted_iota(jnp.int32, (SUBLANES, width), 0)

    low_rows = wide_sublane < 2
    sixth_row = wide_sublane == items
    outer_rows = jnp.logical_or(wide_sublane == 0, wide_sublane >= items)

    def absorb(level, slot, sign):
        first_cell, room = first_buf[level], room_buf[level]
        rows = in_buf[level, slot]

        def spread(i):
            return jnp.broadcast_to(in_buf[level, slot, i : i + 1, :], (SUBLANES, width))

        hot = []
        for piece in range(pieces):
            part = in_buf[level, slot, items:words, piece * LANES : (piece + 1) * LANES].astype(jnp.int32)
            hit = (part - first_cell).astype(jnp.uint32) < room
            hot.append(jnp.where(hit, sign, 0.0))
        hot = jnp.concatenate(hot, axis=1).astype(jnp.bfloat16)
        products = jnp.concatenate(
            [
                jnp.where(sixth_row, spread(5), spread(0)) * jnp.where(sixth_row, pltpu.roll(rows, 1, 0), rows),
                jnp.where(outer_rows, spread(3), spread(1)) * jnp.where(outer_rows, pltpu.roll(rows, 3, 0), rows),
                jnp.where(low_rows, spread(4), spread(2)) * jnp.where(low_rows, pltpu.roll(rows, 4, 0), rows),
                jnp.zeros((SUBLANES, width), jnp.float32),
            ],
            axis=0,
        )
        return lax.dot_general(
            thirds(products), hot, (((1,), (1,)), ((), ())), preferred_element_type=jnp.float32
        )

    height = 4 * SUBLANES

    def gather_level(level, carry):
        totals = [None, None]
        for part, steps in enumerate(batches):
            def batch_rows(count):
                return in_buf.at[level, pl.ds(0, count), pl.ds(0, words)]

            count = len([step for step in steps if step])
            pltpu.make_async_remote_copy(
                src_ref=batch_rows(count), dst_ref=batch_rows(count), send_sem=send_sem,
                recv_sem=recv_sem.at[level, part], device_id=seat_coords(target(1)), device_id_type=MESH,
            ).wait_recv()
            for spot, step in enumerate(steps):
                group, core = origin(step)
                lane = spot % 2
                part_sum = absorb(level, group * CORES + core, 1.0 - 2.0 * lane)
                totals[lane] = part_sum if totals[lane] is None else totals[lane] + part_sum
        total = totals[0] - totals[1]
        total = total[0:height] + total[height : 2 * height] + total[2 * height : 3 * height]
        sums_buf[my_depth, level] = total[0 : 3 * SUBLANES]

        def send_sums(step, carry):
            sums_copy((my_depth + step) % depth, level, my_depth).start()
            return carry

        lax.fori_loop(1, depth, send_sums, 0)
        return carry

    lax.fori_loop(0, depth, gather_level, 0)
    at = {(0, 0): 0, (0, 1): 1, (0, 2): 2, (0, 3): 3, (0, 4): 4, (0, 5): 5, (5, 5): 6,
          (3, 5): 8, (1, 1): 9, (1, 2): 10, (1, 3): 11, (1, 4): 12, (1, 5): 13, (3, 3): 14, (3, 4): 15,
          (4, 4): 16, (4, 5): 17, (2, 2): 18, (2, 3): 19, (2, 4): 20, (2, 5): 21}

    def fit_level(level, carry):
        pltpu.make_async_remote_copy(
            src_ref=sums_buf.at[others, level], dst_ref=sums_buf.at[others, level],
            send_sem=sums_send_sem, recv_sem=sums_recv_sem.at[level],
            device_id=level_coords((my_depth + 1) % depth), device_id_type=MESH,
        ).wait_recv()

        def gather_sums(slot, total):
            return total + sums_buf[slot, level]

        total = lax.fori_loop(1, depth, gather_sums, sums_buf[0, level])

        def entry(i, j):
            spot = at[min(i, j), max(i, j)]
            return total[spot : spot + 1, :]

        normal = [[entry(i, j) for j in range(params)] for i in range(params)]
        moments = [entry(i, params) for i in range(params)]
        with_prior = [[normal[i][j] for j in range(params)] for i in range(params)]
        for i in range(params):
            with_prior[i][i] = normal[i][i] + meta_buf[level, i : i + 1, :]
        updates = solve_rows(with_prior, moments)
        squares = entry(params, params)
        for i in range(params):
            fitted = normal[i][0] * updates[0]
            for j in range(1, params):
                fitted = fitted + normal[i][j] * updates[j]
            squares = squares + updates[i] * (fitted - 2.0 * moments[i])
        counts = meta_buf[level, params:items, :]
        mine = my_group * members + level * CORES + my_core
        tables[mine] = jnp.concatenate(updates + [jnp.full((1, LANES), -1.0, jnp.float32), squares, counts], axis=0)

        def send_table(step, carry):
            table_copy(level, target(plane - 1 - step), mine).start()
            return carry

        lax.fori_loop(0, plane - 1, send_table, 0)
        return carry

    lax.fori_loop(0, depth, fit_level, 0)
    updates_ref[...] = tables[me, 0:params, :]

    def refit_level(level, tails):
        seats = pl.ds(0, plane - 1)
        pltpu.make_async_remote_copy(
            src_ref=tables.at[seats], dst_ref=tables.at[seats],
            send_sem=table_send_sem, recv_sem=table_recv_sem.at[level],
            device_id=seat_coords(target(1)), device_id_type=MESH,
        ).wait_recv()

        for seat in range(plane):
            k = seat // CORES * members + level * CORES + seat % CORES
            table = tables[k]
            tails = tails + table[items : words + 1, :]
            for piece in range(pieces):
                row = pl.ds(k * pieces + piece, 1)
                place = jnp.broadcast_to(place_buf[row, :], (SUBLANES, LANES))
                picked = gather_lanes(table, place)
                rows = out_buf[k, :, piece * LANES : (piece + 1) * LANES]
                fresh = -jnp.sum(jnp.where(sublane < items, picked * rows, 0.0), axis=0, keepdims=True)
                live = rows[words : words + 1, :] < picked[words : words + 1, :]
                root_buf[row, :] = jnp.where(live, fresh, 0.0)
        return tails

    tails = lax.fori_loop(0, depth, refit_level, jnp.zeros((2, LANES), jnp.float32))
    tails = jnp.sum(tails, axis=1, keepdims=True)
    norm = jnp.sqrt(jnp.maximum(tails[0:1], 0.0) / tails[1:2] + 1e-06)
    norm_ref[...] = jnp.broadcast_to(norm, norm_ref.shape)
    scale = 1.0 / norm
    fresh_ref[...] = root_buf[...] * scale

    def drain(ref, semaphore):
        pltpu.make_async_remote_copy(
            src_ref=ref, dst_ref=ref, send_sem=semaphore, recv_sem=meta_recv_sem,
            device_id=seat_coords(target(1)), device_id_type=MESH,
        ).wait_send()

    sent = depth * (plane - 1)
    drain(out_buf.at[pl.ds(0, sent), pl.ds(0, words)], send_sem)
    drain(meta_buf.at[others], meta_send_sem)
    drain(sums_buf.at[others], sums_send_sem)
    drain(tables.at[pl.ds(0, sent)], table_send_sem)


def release(a_ref, b_ref, c_ref, a_out, b_out, c_out, sem):
    pairs = ((a_ref, a_out), (b_ref, b_out), (c_ref, c_out))
    copies = [pltpu.make_async_copy(x, y, sem.at[i]) for i, (x, y) in enumerate(pairs)]
    for copy in copies:
        copy.start()
    for copy in copies:
        copy.wait()


def body(source_id, slot, owner, counts, partials, residual, weight, prior):
    groups, members = lax.axis_size("grp"), lax.axis_size("dev")
    n = groups * members
    params = partials.shape[0]
    row_count = residual.shape[0]
    src_local = counts.shape[0]
    block_rows = row_count // n
    width = -(-block_rows // LANES) * LANES
    depth, plane = members // CORES, groups * CORES

    def lay(array, fill):
        if width == block_rows:
            return array
        blocks = array.reshape(-1, n, block_rows)
        blocks = jnp.pad(blocks, ((0, 0), (0, 0), (0, width - block_rows)), constant_values=fill)
        return blocks.reshape(array.shape[:-1] + (n * width,))

    def dense(array, fill):
        return lay(array, fill).reshape(-1, LANES)

    vmem = pl.BlockSpec(memory_space=pltpu.VMEM)
    operands = (
        dense(source_id, -1),
        dense(slot, 0),
        owner.reshape(-1, LANES),
        counts.reshape(1, src_local),
        lay(partials, 0),
        dense(residual, 0),
        dense(weight, 1),
        prior,
    )
    operands = tuple(pltpu.with_memory_space_constraint(x, pltpu.HBM) for x in operands)
    rows = n * width // LANES
    updates, standardized, norm = pl.pallas_call(
        functools.partial(kernel, (groups, members, width, row_count // src_local)),
        out_shape=(
            pltpu.VMEM((params, src_local), jnp.float32),
            pltpu.VMEM((rows, LANES), jnp.float32),
            pltpu.VMEM((1, LANES), jnp.float32),
        ),
        in_specs=[pl.BlockSpec(memory_space=pltpu.HBM)] * len(operands),
        out_specs=(vmem, vmem, vmem),
        scratch_shapes=[pltpu.VMEM(operand.shape, operand.dtype) for operand in operands] + [
            pltpu.VMEM((rows, LANES), jnp.float32),
            pltpu.VMEM((rows, LANES), jnp.float32),
            pltpu.VMEM((rows, LANES), jnp.int32),
            pltpu.VMEM((n, SUBLANES, width), jnp.float32),
            pltpu.VMEM((depth, plane, SUBLANES, width), jnp.float32),
            pltpu.VMEM((depth, SUBLANES, LANES), jnp.float32),
            pltpu.VMEM((depth, src_local, LANES), jnp.int32),
            pltpu.VMEM((depth, src_local, LANES), jnp.uint32),
            pltpu.VMEM((depth, depth, 3 * SUBLANES, LANES), jnp.float32),
            pltpu.VMEM((n, SUBLANES, LANES), jnp.float32),
            pltpu.SemaphoreType.DMA((len(operands),)),
            pltpu.SemaphoreType.DMA,
            pltpu.SemaphoreType.DMA((depth, 2)),
            pltpu.SemaphoreType.DMA,
            pltpu.SemaphoreType.DMA,
            pltpu.SemaphoreType.DMA,
            pltpu.SemaphoreType.DMA((depth,)),
            pltpu.SemaphoreType.DMA,
            pltpu.SemaphoreType.DMA((depth,)),
        ],
        compiler_params=pltpu.CompilerParams(
            collective_id=0, has_side_effects=True, vmem_limit_bytes=40 << 20
        ),
        name="exchange_fit",
    )(*operands)
    results = (updates, standardized, norm)
    updates, standardized, norm = pl.pallas_call(
        release,
        out_shape=tuple(jax.ShapeDtypeStruct(r.shape, r.dtype) for r in results),
        in_specs=[vmem] * 3,
        out_specs=[pl.BlockSpec(memory_space=pltpu.HBM)] * 3,
        scratch_shapes=[pltpu.SemaphoreType.DMA((3,))],
        compiler_params=pltpu.CompilerParams(vmem_limit_bytes=4 << 20),
        name="release",
    )(*results)
    standardized = standardized.reshape(n, width)[:, :block_rows] if width != block_rows else standardized
    return (updates, standardized.reshape(row_count), norm[0, 0])


def solution(mesh):
    in_specs = (
        P(("grp", "dev")),
        P(("grp", "dev")),
        P(),
        P(("grp", "dev")),
        P(None, ("grp", "dev")),
        P(("grp", "dev")),
        P(("grp", "dev")),
        P(None, ("grp", "dev")),
    )
    out_specs = (P(None, ("grp", "dev")), P(("grp", "dev")), P())
    return jax.shard_map(body, mesh=mesh, in_specs=in_specs, out_specs=out_specs, check_vma=False)
```

```python
import functools

import jax
import jax.numpy as jnp
from jax import lax
from jax.experimental import pallas as pl
from jax.experimental.pallas import tpu as pltpu
from jax.sharding import PartitionSpec as P

LANES = 128
SUBLANES = 8
CORES = 2
MESH = pl.DeviceIdType.MESH


def solve_rows(normal, moments):
    params = len(moments)
    factor = {}
    inverse = []
    for column in range(params):
        running = normal[column][column]
        for earlier in range(column):
            running = running - factor[column, earlier] ** 2
        inverse.append(1.0 / jnp.sqrt(running))
        for target in range(column + 1, params):
            current = normal[target][column]
            for earlier in range(column):
                current = current - factor[target, earlier] * factor[column, earlier]
            factor[target, column] = current * inverse[column]
    forward = []
    for target in range(params):
        current = moments[target]
        for earlier in range(target):
            current = current - factor[target, earlier] * forward[earlier]
        forward.append(current * inverse[target])
    backward = [None] * params
    for target in reversed(range(params)):
        current = forward[target]
        for later in range(target + 1, params):
            current = current - factor[later, target] * backward[later]
        backward[target] = current * inverse[target]
    return backward


def thirds(values):
    high = values.astype(jnp.bfloat16)
    rest = values - high.astype(jnp.float32)
    middle = rest.astype(jnp.bfloat16)
    last = (rest - middle.astype(jnp.float32)).astype(jnp.bfloat16)
    return jnp.concatenate([high, middle, last], axis=0)


def gather_lanes(table, index):
    return jnp.take_along_axis(table, index, axis=1, mode="promise_in_bounds")


def kernel(
    sizes,
    source_hbm, slot_hbm, owner_hbm, counts_hbm, partials_hbm, residual_hbm, weight_hbm, prior_hbm,
    updates_ref, fresh_ref, norm_ref,
    source_ref, slot_ref, owner_ref, counts_ref, partials_ref, residual_ref, weight_ref, prior_ref,
    root_buf, cell_buf, place_buf, out_buf, in_buf, meta_buf, first_buf, room_buf, sums_buf, tables,
    load_sem, send_sem, recv_sem, meta_send_sem, meta_recv_sem, sums_send_sem, sums_recv_sem,
    table_send_sem, table_recv_sem,
):
    groups, members, width, pad_slots = sizes
    n = groups * members
    params = partials_ref.shape[0]
    words = params + 2
    items = params + 1
    depth = members // CORES
    plane = groups * CORES
    pieces = width // LANES
    low = 2 if groups % 2 == 0 else 1
    high = groups // low
    row_pairs = (
        (owner_hbm, owner_ref), (source_hbm, source_ref), (slot_hbm, slot_ref), (weight_hbm, weight_ref),
        (residual_hbm, residual_ref), (partials_hbm, partials_ref), (counts_hbm, counts_ref), (prior_hbm, prior_ref),
    )
    loads = [pltpu.make_async_copy(a, b, load_sem.at[i]) for i, (a, b) in enumerate(row_pairs)]
    for load in loads:
        load.start()
    my_group, my_member = lax.axis_index("grp"), lax.axis_index("dev")
    my_depth, my_core = my_member // CORES, my_member % CORES
    me = my_group * members + my_member
    my_seat = my_group * CORES + my_core

    def target(step):
        jump = step // CORES
        group = (my_group // low + jump // low) % high * low + (my_group % low + jump % low) % low
        return group, (my_core + step % CORES) % CORES

    def origin(step):
        jump = step // CORES
        group = (my_group // low + high - jump // low) % high * low + (my_group % low + low - jump % low) % low
        return group, (my_core + CORES - step % CORES) % CORES

    def seat_coords(seat):
        group, core = seat
        return (group, my_depth * CORES + core)

    def level_coords(level):
        return (my_group, level * CORES + my_core)

    barrier = pltpu.get_barrier_semaphore()
    few = depth <= 4
    used = 3 * SUBLANES - 2

    def greet_level(step, carry):
        pl.semaphore_signal(barrier, inc=1, device_id=level_coords((my_depth + step) % depth), device_id_type=MESH)
        return carry

    lax.fori_loop(1, depth, greet_level, 0, unroll=few)
    for step in range(plane - 1, 0, -1):
        pl.semaphore_signal(barrier, inc=1, device_id=seat_coords(target(step)), device_id_type=MESH)

    for load in loads:
        load.wait()

    root = jnp.sqrt(weight_ref[...])
    root_buf[...] = root
    residual_ref[...] = residual_ref[...] * root
    cell_buf[...] = (source_ref[...] * pad_slots + slot_ref[...]).astype(jnp.float32)

    sublane = lax.broadcasted_iota(jnp.int32, (SUBLANES, LANES), 0)

    def prepare(level, seat, carry):
        k = seat // CORES * members + level * CORES + seat % CORES
        for piece in range(pieces):
            row = pl.ds(k * pieces + piece, 1)
            cols = pl.ds(pl.multiple_of(k * width + piece * LANES, LANES), LANES)

            def spread(ref):
                return jnp.broadcast_to(ref[row, :], (SUBLANES, LANES))

            scaled = partials_ref[:, cols] * jnp.broadcast_to(root_buf[row, :], (params, LANES))
            part = slice(piece * LANES, (piece + 1) * LANES)
            out_buf[k, 0:params, part] = scaled
            out_buf[k, params:items, part] = residual_ref[row, :]
            out_buf[k, items:words, part] = cell_buf[row, :]
            out_buf[k, words : words + 1, part] = slot_ref[row, :].astype(jnp.float32)
        return carry

    def prepare_level(level, carry):
        return lax.fori_loop(0, plane, functools.partial(prepare, level), carry, unroll=2)

    prepare_level(0, 0)

    pl.semaphore_wait(barrier, plane - 1 + depth - 1)

    def meta_copy(level, slot):
        return pltpu.make_async_remote_copy(
            src_ref=meta_buf.at[slot], dst_ref=meta_buf.at[slot], send_sem=meta_send_sem, recv_sem=meta_recv_sem,
            device_id=level_coords(level), device_id_type=MESH,
        )

    def row_copy(level, seat, slot, part):
        group, core = seat
        return pltpu.make_async_remote_copy(
            src_ref=out_buf.at[group * members + level * CORES + core, pl.ds(0, words)],
            dst_ref=in_buf.at[level, slot, pl.ds(0, words)],
            send_sem=send_sem, recv_sem=recv_sem.at[level, part],
            device_id=seat_coords(seat), device_id_type=MESH,
        )

    def sums_copy(level, stage, slot):
        return pltpu.make_async_remote_copy(
            src_ref=sums_buf.at[slot, stage, pl.ds(0, used)], dst_ref=sums_buf.at[slot, stage, pl.ds(0, used)],
            send_sem=sums_send_sem, recv_sem=sums_recv_sem.at[stage],
            device_id=level_coords(level), device_id_type=MESH,
        )

    def table_copy(stage, seat, slot):
        return pltpu.make_async_remote_copy(
            src_ref=tables.at[slot], dst_ref=tables.at[slot],
            send_sem=table_send_sem, recv_sem=table_recv_sem.at[stage],
            device_id=seat_coords(seat), device_id_type=MESH,
        )

    half = plane // 2
    batches = ([0] + list(range(plane - 1, half, -1)), list(range(half, 0, -1)))

    def send_rows(level):
        for part, steps in enumerate(batches):
            for step in steps:
                if step:
                    row_copy(level, target(step), my_seat, part).start()

    def stream_rows(level, carry):
        prepare_level(level, 0)
        send_rows(level - 1)
        return carry

    lax.fori_loop(1, depth, stream_rows, 0)
    send_rows(depth - 1)

    def own_rows(level, carry):
        in_buf[level, my_seat] = out_buf[my_group * members + level * CORES + my_core]
        return carry

    lax.fori_loop(0, depth, own_rows, 0)

    src_local = counts_ref.shape[1]
    square = (src_local, LANES)
    row_index = lax.broadcasted_iota(jnp.int32, square, 0)
    lane_index = lax.broadcasted_iota(jnp.int32, square, 1)
    diagonal = row_index == lane_index

    spare = 4

    def invert(step, total):
        for part in range(spare):
            tile = step * spare + part
            ids = tile * LANES + lane_index
            total = jnp.where(owner_ref[pl.ds(tile, 1), :] == row_index + me * src_local, ids, total)
        return total

    found = lax.fori_loop(0, owner_ref.shape[0] // spare, invert, jnp.zeros(square, jnp.int32))
    source_at = jnp.sum(found.astype(jnp.float32), axis=1, keepdims=True)
    source_at = jnp.sum(jnp.where(diagonal, source_at, 0.0), axis=0, keepdims=True)
    meta_buf[my_depth] = jnp.concatenate(
        [prior_ref[...], counts_ref[...].astype(jnp.float32), source_at * pad_slots]
        + [jnp.zeros((SUBLANES - words, LANES), jnp.float32)],
        axis=0,
    )

    def send_meta(step, carry):
        meta_copy((my_depth + step) % depth, my_depth).start()
        return carry

    lax.fori_loop(1, depth, send_meta, 0)

    batch = min(32, owner_ref.shape[0])

    def locate(step, carry):
        rows = pl.ds(pl.multiple_of(step * SUBLANES, SUBLANES), SUBLANES)
        source = source_ref[rows, :]
        lane, tile = source % LANES, source // LANES

        def look(group, found):
            for t in range(batch):
                row = group * batch + t
                entry = jnp.broadcast_to(owner_ref[pl.ds(row, 1), :], (SUBLANES, LANES))
                found = jnp.where(tile == row, gather_lanes(entry, lane), found)
            return found

        found = jnp.full((SUBLANES, LANES), -1, jnp.int32)
        if owner_ref.shape[0] == batch:
            found = look(0, found)
        else:
            found = lax.fori_loop(0, owner_ref.shape[0] // batch, look, found)
        place_buf[rows, :] = found % LANES
        return carry

    lax.fori_loop(0, source_ref.shape[0] // SUBLANES, locate, 0)


    others = pl.ds(0, depth - 1)
    pltpu.make_async_remote_copy(
        src_ref=meta_buf.at[others], dst_ref=meta_buf.at[others], send_sem=meta_send_sem, recv_sem=meta_recv_sem,
        device_id=level_coords((my_depth + 1) % depth), device_id_type=MESH,
    ).wait_recv()

    def find_cells(level, carry):
        first, counts = meta_buf[level, items:words, :], meta_buf[level, params:items, :]
        first = jnp.sum(jnp.where(diagonal, first, 0.0), axis=1, keepdims=True)
        counts = jnp.sum(jnp.where(diagonal, counts, 0.0), axis=1, keepdims=True)
        first_buf[level] = jnp.broadcast_to(first, square).astype(jnp.int32)
        room_buf[level] = jnp.broadcast_to(counts, square).astype(jnp.int32).astype(jnp.uint32)
        return carry

    lax.fori_loop(0, depth, find_cells, 0, unroll=depth if depth <= 4 else 1)
    wide_sublane = lax.broadcasted_iota(jnp.int32, (SUBLANES, width), 0)

    low_rows = wide_sublane < 2
    sixth_row = wide_sublane == items
    outer_rows = jnp.logical_or(wide_sublane == 0, wide_sublane >= items)

    def absorb(level, slot, sign):
        first_cell, room = first_buf[level], room_buf[level]
        rows = in_buf[level, slot]

        def spread(i):
            return jnp.broadcast_to(in_buf[level, slot, i : i + 1, :], (SUBLANES, width))

        hot = []
        for piece in range(pieces):
            part = in_buf[level, slot, items:words, piece * LANES : (piece + 1) * LANES].astype(jnp.int32)
            hit = (part - first_cell).astype(jnp.uint32) < room
            hot.append(jnp.where(hit, sign, 0.0))
        hot = jnp.concatenate(hot, axis=1).astype(jnp.bfloat16)
        products = jnp.concatenate(
            [
                jnp.where(sixth_row, spread(5), spread(0)) * jnp.where(sixth_row, pltpu.roll(rows, 1, 0), rows),
                jnp.where(outer_rows, spread(3), spread(1)) * jnp.where(outer_rows, pltpu.roll(rows, 3, 0), rows),
                jnp.where(low_rows, spread(4), spread(2)) * jnp.where(low_rows, pltpu.roll(rows, 4, 0), rows),
                jnp.zeros((SUBLANES, width), jnp.float32),
            ],
            axis=0,
        )
        return lax.dot_general(
            thirds(products), hot, (((1,), (1,)), ((), ())), preferred_element_type=jnp.float32
        )

    height = 4 * SUBLANES

    def gather_level(level, carry):
        totals = [None, None]
        for part, steps in enumerate(batches):
            def batch_rows(count):
                return in_buf.at[level, pl.ds(0, count), pl.ds(0, words)]

            count = len([step for step in steps if step])
            pltpu.make_async_remote_copy(
                src_ref=batch_rows(count), dst_ref=batch_rows(count), send_sem=send_sem,
                recv_sem=recv_sem.at[level, part], device_id=seat_coords(target(1)), device_id_type=MESH,
            ).wait_recv()
            for spot, step in enumerate(steps):
                group, core = origin(step)
                lane = spot % 2
                part_sum = absorb(level, group * CORES + core, 1.0 - 2.0 * lane)
                totals[lane] = part_sum if totals[lane] is None else totals[lane] + part_sum
        total = totals[0] - totals[1]
        total = total[0:height] + total[height : 2 * height] + total[2 * height : 3 * height]
        sums_buf[my_depth, level] = total[0 : 3 * SUBLANES]

        def send_sums(step, carry):
            sums_copy((my_depth + step) % depth, level, my_depth).start()
            return carry

        lax.fori_loop(1, depth, send_sums, 0, unroll=few)
        return carry

    lax.fori_loop(0, depth, gather_level, 0)
    at = {(0, 0): 0, (0, 1): 1, (0, 2): 2, (0, 3): 3, (0, 4): 4, (0, 5): 5, (5, 5): 6,
          (3, 5): 8, (1, 1): 9, (1, 2): 10, (1, 3): 11, (1, 4): 12, (1, 5): 13, (3, 3): 14, (3, 4): 15,
          (4, 4): 16, (4, 5): 17, (2, 2): 18, (2, 3): 19, (2, 4): 20, (2, 5): 21}

    def fit_level(level, carry):
        pltpu.make_async_remote_copy(
            src_ref=sums_buf.at[others, level, pl.ds(0, used)], dst_ref=sums_buf.at[others, level, pl.ds(0, used)],
            send_sem=sums_send_sem, recv_sem=sums_recv_sem.at[level],
            device_id=level_coords((my_depth + 1) % depth), device_id_type=MESH,
        ).wait_recv()

        def gather_sums(slot, total):
            return total + sums_buf[slot, level, 0:used, :]

        total = lax.fori_loop(1, depth, gather_sums, sums_buf[0, level, 0:used, :], unroll=few)

        def entry(i, j):
            spot = at[min(i, j), max(i, j)]
            return total[spot : spot + 1, :]

        normal = [[entry(i, j) for j in range(params)] for i in range(params)]
        moments = [entry(i, params) for i in range(params)]
        with_prior = [[normal[i][j] for j in range(params)] for i in range(params)]
        for i in range(params):
            with_prior[i][i] = normal[i][i] + meta_buf[level, i : i + 1, :]
        updates = solve_rows(with_prior, moments)
        squares = entry(params, params)
        for i in range(params):
            fitted = normal[i][0] * updates[0]
            for j in range(1, params):
                fitted = fitted + normal[i][j] * updates[j]
            squares = squares + updates[i] * (fitted - 2.0 * moments[i])
        counts = meta_buf[level, params:items, :]
        mine = my_group * members + level * CORES + my_core
        tables[mine] = jnp.concatenate(updates + [jnp.full((1, LANES), -1.0, jnp.float32), squares, counts], axis=0)

        for step in range(plane - 1, 0, -1):
            table_copy(level, target(step), mine).start()
        return carry

    lax.fori_loop(0, depth, fit_level, 0)
    updates_ref[...] = tables[me, 0:params, :]

    def drain(ref, semaphore):
        pltpu.make_async_remote_copy(
            src_ref=ref, dst_ref=ref, send_sem=semaphore, recv_sem=meta_recv_sem,
            device_id=seat_coords(target(1)), device_id_type=MESH,
        ).wait_send()

    def refit_level(level, tails):
        seats = pl.ds(0, plane - 1)
        pltpu.make_async_remote_copy(
            src_ref=tables.at[seats], dst_ref=tables.at[seats],
            send_sem=table_send_sem, recv_sem=table_recv_sem.at[level],
            device_id=seat_coords(target(1)), device_id_type=MESH,
        ).wait_recv()

        for seat in range(plane):
            k = seat // CORES * members + level * CORES + seat % CORES
            table = tables[k]
            tails = tails + table[items : words + 1, :]
            for piece in range(pieces):
                row = pl.ds(k * pieces + piece, 1)
                place = jnp.broadcast_to(place_buf[row, :], (SUBLANES, LANES))
                picked = gather_lanes(table, place)
                rows = out_buf[k, :, piece * LANES : (piece + 1) * LANES]
                fresh = -jnp.sum(jnp.where(sublane < items, picked * rows, 0.0), axis=0, keepdims=True)
                live = rows[words : words + 1, :] < picked[words : words + 1, :]
                root_buf[row, :] = jnp.where(live, fresh, 0.0)
        return tails

    tails = lax.fori_loop(0, depth - 1, refit_level, jnp.zeros((2, LANES), jnp.float32))
    sent = depth * (plane - 1)
    drain(out_buf.at[pl.ds(0, sent), pl.ds(0, words)], send_sem)
    drain(meta_buf.at[others], meta_send_sem)
    drain(sums_buf.at[others, :, pl.ds(0, used)], sums_send_sem)
    tails = refit_level(depth - 1, tails)
    tails = jnp.sum(tails, axis=1, keepdims=True)
    norm = jnp.sqrt(jnp.maximum(tails[0:1], 0.0) / tails[1:2] + 1e-06)
    norm_ref[...] = jnp.broadcast_to(norm, norm_ref.shape)
    scale = 1.0 / norm
    fresh_ref[...] = root_buf[...] * scale

    drain(tables.at[pl.ds(0, sent)], table_send_sem)


def release(a_ref, b_ref, c_ref, a_out, b_out, c_out, sem):
    pairs = ((a_ref, a_out), (b_ref, b_out), (c_ref, c_out))
    copies = [pltpu.make_async_copy(x, y, sem.at[i]) for i, (x, y) in enumerate(pairs)]
    for copy in copies:
        copy.start()
    for copy in copies:
        copy.wait()


def body(source_id, slot, owner, counts, partials, residual, weight, prior):
    groups, members = lax.axis_size("grp"), lax.axis_size("dev")
    n = groups * members
    params = partials.shape[0]
    row_count = residual.shape[0]
    src_local = counts.shape[0]
    block_rows = row_count // n
    width = -(-block_rows // LANES) * LANES
    depth, plane = members // CORES, groups * CORES

    def lay(array, fill):
        if width == block_rows:
            return array
        blocks = array.reshape(-1, n, block_rows)
        blocks = jnp.pad(blocks, ((0, 0), (0, 0), (0, width - block_rows)), constant_values=fill)
        return blocks.reshape(array.shape[:-1] + (n * width,))

    def dense(array, fill):
        return lay(array, fill).reshape(-1, LANES)

    vmem = pl.BlockSpec(memory_space=pltpu.VMEM)
    operands = (
        dense(source_id, -1),
        dense(slot, 0),
        owner.reshape(-1, LANES),
        counts.reshape(1, src_local),
        lay(partials, 0),
        dense(residual, 0),
        dense(weight, 1),
        prior,
    )
    operands = tuple(pltpu.with_memory_space_constraint(x, pltpu.HBM) for x in operands)
    rows = n * width // LANES
    updates, standardized, norm = pl.pallas_call(
        functools.partial(kernel, (groups, members, width, row_count // src_local)),
        out_shape=(
            pltpu.VMEM((params, src_local), jnp.float32),
            pltpu.VMEM((rows, LANES), jnp.float32),
            pltpu.VMEM((1, LANES), jnp.float32),
        ),
        in_specs=[pl.BlockSpec(memory_space=pltpu.HBM)] * len(operands),
        out_specs=(vmem, vmem, vmem),
        scratch_shapes=[pltpu.VMEM(operand.shape, operand.dtype) for operand in operands] + [
            pltpu.VMEM((rows, LANES), jnp.float32),
            pltpu.VMEM((rows, LANES), jnp.float32),
            pltpu.VMEM((rows, LANES), jnp.int32),
            pltpu.VMEM((n, SUBLANES, width), jnp.float32),
            pltpu.VMEM((depth, plane, SUBLANES, width), jnp.float32),
            pltpu.VMEM((depth, SUBLANES, LANES), jnp.float32),
            pltpu.VMEM((depth, src_local, LANES), jnp.int32),
            pltpu.VMEM((depth, src_local, LANES), jnp.uint32),
            pltpu.VMEM((depth, depth, 3 * SUBLANES, LANES), jnp.float32),
            pltpu.VMEM((n, SUBLANES, LANES), jnp.float32),
            pltpu.SemaphoreType.DMA((len(operands),)),
            pltpu.SemaphoreType.DMA,
            pltpu.SemaphoreType.DMA((depth, 2)),
            pltpu.SemaphoreType.DMA,
            pltpu.SemaphoreType.DMA,
            pltpu.SemaphoreType.DMA,
            pltpu.SemaphoreType.DMA((depth,)),
            pltpu.SemaphoreType.DMA,
            pltpu.SemaphoreType.DMA((depth,)),
        ],
        compiler_params=pltpu.CompilerParams(
            collective_id=0, has_side_effects=True, vmem_limit_bytes=40 << 20
        ),
        name="exchange_fit",
    )(*operands)
    results = (updates, standardized, norm)
    updates, standardized, norm = pl.pallas_call(
        release,
        out_shape=tuple(jax.ShapeDtypeStruct(r.shape, r.dtype) for r in results),
        in_specs=[vmem] * 3,
        out_specs=[pl.BlockSpec(memory_space=pltpu.HBM)] * 3,
        scratch_shapes=[pltpu.SemaphoreType.DMA((3,))],
        compiler_params=pltpu.CompilerParams(vmem_limit_bytes=4 << 20),
        name="release",
    )(*results)
    standardized = standardized.reshape(n, width)[:, :block_rows] if width != block_rows else standardized
    return (updates, standardized.reshape(row_count), norm[0, 0])


def solution(mesh):
    in_specs = (
        P(("grp", "dev")),
        P(("grp", "dev")),
        P(),
        P(("grp", "dev")),
        P(None, ("grp", "dev")),
        P(("grp", "dev")),
        P(("grp", "dev")),
        P(None, ("grp", "dev")),
    )
    out_specs = (P(None, ("grp", "dev")), P(("grp", "dev")), P())
    return jax.shard_map(body, mesh=mesh, in_specs=in_specs, out_specs=out_specs, check_vma=False)
```

```python
import functools

import jax
import jax.numpy as jnp
from jax import lax
from jax.experimental import pallas as pl
from jax.experimental.pallas import tpu as pltpu
from jax.sharding import PartitionSpec as P

LANES = 128
SUBLANES = 8
CORES = 2
MESH = pl.DeviceIdType.MESH


def solve_rows(normal, moments):
    params = len(moments)
    factor = {}
    inverse = []
    for column in range(params):
        running = normal[column][column]
        for earlier in range(column):
            running = running - factor[column, earlier] ** 2
        inverse.append(1.0 / jnp.sqrt(running))
        for target in range(column + 1, params):
            current = normal[target][column]
            for earlier in range(column):
                current = current - factor[target, earlier] * factor[column, earlier]
            factor[target, column] = current * inverse[column]
    forward = []
    for target in range(params):
        current = moments[target]
        for earlier in range(target):
            current = current - factor[target, earlier] * forward[earlier]
        forward.append(current * inverse[target])
    backward = [None] * params
    for target in reversed(range(params)):
        current = forward[target]
        for later in range(target + 1, params):
            current = current - factor[later, target] * backward[later]
        backward[target] = current * inverse[target]
    return backward


def thirds(values):
    high = values.astype(jnp.bfloat16)
    rest = values - high.astype(jnp.float32)
    middle = rest.astype(jnp.bfloat16)
    last = (rest - middle.astype(jnp.float32)).astype(jnp.bfloat16)
    return jnp.concatenate([high, middle, last], axis=0)


def gather_lanes(table, index):
    return jnp.take_along_axis(table, index, axis=1, mode="promise_in_bounds")


def kernel(
    sizes,
    source_hbm, slot_hbm, owner_hbm, counts_hbm, partials_hbm, residual_hbm, weight_hbm, prior_hbm,
    updates_ref, fresh_ref, norm_ref,
    source_ref, slot_ref, owner_ref, counts_ref, partials_ref, residual_ref, weight_ref, prior_ref,
    root_buf, cell_buf, place_buf, out_buf, in_buf, meta_buf, first_buf, room_buf, sums_buf, tables,
    load_sem, send_sem, recv_sem, meta_send_sem, meta_recv_sem, meta_lead_sem, sums_send_sem, sums_recv_sem,
    table_send_sem, table_recv_sem,
):
    groups, members, width, pad_slots = sizes
    n = groups * members
    params = partials_ref.shape[0]
    words = params + 2
    items = params + 1
    depth = members // CORES
    plane = groups * CORES
    pieces = width // LANES
    low = 2 if groups % 2 == 0 else 1
    high = groups // low
    row_pairs = (
        (owner_hbm, owner_ref), (source_hbm, source_ref), (slot_hbm, slot_ref), (weight_hbm, weight_ref),
        (residual_hbm, residual_ref), (partials_hbm, partials_ref), (counts_hbm, counts_ref), (prior_hbm, prior_ref),
    )
    loads = [pltpu.make_async_copy(a, b, load_sem.at[i]) for i, (a, b) in enumerate(row_pairs)]
    for load in loads:
        load.start()
    my_group, my_member = lax.axis_index("grp"), lax.axis_index("dev")
    my_depth, my_core = my_member // CORES, my_member % CORES
    me = my_group * members + my_member
    my_seat = my_group * CORES + my_core

    def target(step):
        jump = step // CORES
        group = (my_group // low + jump // low) % high * low + (my_group % low + jump % low) % low
        return group, (my_core + step % CORES) % CORES

    def origin(step):
        jump = step // CORES
        group = (my_group // low + high - jump // low) % high * low + (my_group % low + low - jump % low) % low
        return group, (my_core + CORES - step % CORES) % CORES

    def seat_coords(seat):
        group, core = seat
        return (group, my_depth * CORES + core)

    def level_coords(level, core=None):
        return (my_group, level * CORES + (my_core if core is None else core))

    lead = CORES - 1

    barrier = pltpu.get_barrier_semaphore()
    few = depth <= 4
    used = 3 * SUBLANES - 2

    def greet_level(step, carry):
        level = (my_depth + step) % depth
        pl.semaphore_signal(barrier, inc=1, device_id=level_coords(level), device_id_type=MESH)
        return carry

    def greet_follower(step, carry):
        level = (my_depth + step) % depth
        pl.semaphore_signal(barrier, inc=1, device_id=level_coords(level, 0), device_id_type=MESH)
        return carry

    lax.fori_loop(1, depth, greet_level, 0, unroll=few)
    lax.fori_loop(jnp.where(my_core == lead, 1, depth), depth, greet_follower, 0)
    for step in range(plane - 1, 0, -1):
        pl.semaphore_signal(barrier, inc=1, device_id=seat_coords(target(step)), device_id_type=MESH)

    for load in loads:
        load.wait()

    meta_buf[my_core * depth + my_depth] = jnp.concatenate(
        [prior_ref[...], counts_ref[...].astype(jnp.float32), jnp.zeros((SUBLANES - items, LANES), jnp.float32)], axis=0
    )
    root = jnp.sqrt(weight_ref[...])
    root_buf[...] = root
    residual_ref[...] = residual_ref[...] * root
    cell_buf[...] = (source_ref[...] * pad_slots + slot_ref[...]).astype(jnp.float32)

    sublane = lax.broadcasted_iota(jnp.int32, (SUBLANES, LANES), 0)

    def prepare(level, seat, carry):
        k = seat // CORES * members + level * CORES + seat % CORES
        for piece in range(pieces):
            row = pl.ds(k * pieces + piece, 1)
            cols = pl.ds(pl.multiple_of(k * width + piece * LANES, LANES), LANES)

            def spread(ref):
                return jnp.broadcast_to(ref[row, :], (SUBLANES, LANES))

            scaled = partials_ref[:, cols] * jnp.broadcast_to(root_buf[row, :], (params, LANES))
            part = slice(piece * LANES, (piece + 1) * LANES)
            out_buf[k, 0:params, part] = scaled
            out_buf[k, params:items, part] = residual_ref[row, :]
            out_buf[k, items:words, part] = cell_buf[row, :]
            out_buf[k, words : words + 1, part] = slot_ref[row, :].astype(jnp.float32)
        return carry

    def prepare_level(level, carry):
        return lax.fori_loop(0, plane, functools.partial(prepare, level), carry, unroll=2)

    prepare_level(0, 0)

    pl.semaphore_wait(barrier, plane - 1 + (depth - 1) * (CORES - my_core))

    def meta_copy(level, core, semaphore):
        slot = my_core * depth + my_depth
        return pltpu.make_async_remote_copy(
            src_ref=meta_buf.at[slot], dst_ref=meta_buf.at[slot], send_sem=meta_send_sem, recv_sem=semaphore,
            device_id=level_coords(level, core), device_id_type=MESH,
        )

    def row_copy(level, seat, slot, part):
        group, core = seat
        return pltpu.make_async_remote_copy(
            src_ref=out_buf.at[group * members + level * CORES + core, pl.ds(0, words)],
            dst_ref=in_buf.at[level, slot, pl.ds(0, words)],
            send_sem=send_sem, recv_sem=recv_sem.at[level, part],
            device_id=seat_coords(seat), device_id_type=MESH,
        )

    def sums_copy(level, stage):
        slot = my_core * depth + my_depth
        return pltpu.make_async_remote_copy(
            src_ref=sums_buf.at[slot, stage, pl.ds(0, used)], dst_ref=sums_buf.at[slot, stage, pl.ds(0, used)],
            send_sem=sums_send_sem, recv_sem=sums_recv_sem.at[stage],
            device_id=level_coords(level, lead), device_id_type=MESH,
        )

    def table_copy(stage, seat):
        pair = pl.ds(my_group * members + stage * CORES, CORES)
        return pltpu.make_async_remote_copy(
            src_ref=tables.at[pair], dst_ref=tables.at[pair],
            send_sem=table_send_sem, recv_sem=table_recv_sem.at[stage],
            device_id=seat_coords(seat), device_id_type=MESH,
        )

    def send_meta(step, carry):
        meta_copy((my_depth + step) % depth, my_core, meta_recv_sem).start()
        return carry

    def send_meta_lead(step, carry):
        meta_copy((my_depth + step) % depth, lead, meta_lead_sem).start()
        return carry

    lax.fori_loop(1, depth, send_meta, 0, unroll=few)

    half = plane // 2
    batches = ([0] + list(range(plane - 1, half, -1)), list(range(half, 0, -1)))

    def send_rows(level):
        for part, steps in enumerate(batches):
            for step in steps:
                if step:
                    row_copy(level, target(step), my_seat, part).start()

    def stream_rows(level, carry):
        prepare_level(level, 0)
        send_rows(level - 1)
        return carry

    lax.fori_loop(1, depth, stream_rows, 0)
    send_rows(depth - 1)
    lax.fori_loop(0, jnp.where(my_core == lead, 0, depth), send_meta_lead, 0)

    def own_rows(level, carry):
        in_buf[level, my_seat] = out_buf[my_group * members + level * CORES + my_core]
        return carry

    lax.fori_loop(0, depth, own_rows, 0)

    src_local = counts_ref.shape[1]
    square = (src_local, LANES)
    row_index = lax.broadcasted_iota(jnp.int32, square, 0)
    lane_index = lax.broadcasted_iota(jnp.int32, square, 1)
    diagonal = row_index == lane_index
    spare = 4

    def invert(level, carry):
        position = (my_group * members + level * CORES + my_core) * src_local + row_index

        def scan(step, total):
            for part in range(spare):
                tile = step * spare + part
                total = jnp.where(owner_ref[pl.ds(tile, 1), :] == position, tile * LANES + lane_index, total)
            return total

        found = lax.fori_loop(0, owner_ref.shape[0] // spare, scan, jnp.zeros(square, jnp.int32))
        source_at = jnp.sum(found.astype(jnp.float32), axis=1, keepdims=True)
        first_buf[level] = jnp.broadcast_to(source_at * pad_slots, square).astype(jnp.int32)
        return carry

    lax.fori_loop(0, depth, invert, 0)

    others = pl.ds(0, depth - 1)
    pltpu.make_async_remote_copy(
        src_ref=meta_buf.at[others], dst_ref=meta_buf.at[others], send_sem=meta_send_sem, recv_sem=meta_recv_sem,
        device_id=level_coords((my_depth + 1) % depth), device_id_type=MESH,
    ).wait_recv()

    def find_room(level, carry):
        counts = meta_buf[my_core * depth + level, params:items, :]
        counts = jnp.sum(jnp.where(diagonal, counts, 0.0), axis=1, keepdims=True)
        room_buf[level] = jnp.broadcast_to(counts, square).astype(jnp.int32).astype(jnp.uint32)
        return carry

    lax.fori_loop(0, depth, find_room, 0, unroll=few)
    wide_sublane = lax.broadcasted_iota(jnp.int32, (SUBLANES, width), 0)

    low_rows = wide_sublane < 2
    sixth_row = wide_sublane == items
    outer_rows = jnp.logical_or(wide_sublane == 0, wide_sublane >= items)

    def absorb(level, slot, sign):
        first_cell, room = first_buf[level], room_buf[level]
        rows = in_buf[level, slot]

        def spread(i):
            return jnp.broadcast_to(in_buf[level, slot, i : i + 1, :], (SUBLANES, width))

        hot = []
        for piece in range(pieces):
            part = in_buf[level, slot, items:words, piece * LANES : (piece + 1) * LANES].astype(jnp.int32)
            hit = (part - first_cell).astype(jnp.uint32) < room
            hot.append(jnp.where(hit, sign, 0.0))
        hot = jnp.concatenate(hot, axis=1).astype(jnp.bfloat16)
        products = jnp.concatenate(
            [
                jnp.where(sixth_row, spread(5), spread(0)) * jnp.where(sixth_row, pltpu.roll(rows, 1, 0), rows),
                jnp.where(outer_rows, spread(3), spread(1)) * jnp.where(outer_rows, pltpu.roll(rows, 3, 0), rows),
                jnp.where(low_rows, spread(4), spread(2)) * jnp.where(low_rows, pltpu.roll(rows, 4, 0), rows),
                jnp.zeros((SUBLANES, width), jnp.float32),
            ],
            axis=0,
        )
        return lax.dot_general(
            thirds(products), hot, (((1,), (1,)), ((), ())), preferred_element_type=jnp.float32
        )

    height = 4 * SUBLANES

    def gather_level(level, carry):
        totals = [None, None]
        for part, steps in enumerate(batches):
            def batch_rows(count):
                return in_buf.at[level, pl.ds(0, count), pl.ds(0, words)]

            count = len([step for step in steps if step])
            pltpu.make_async_remote_copy(
                src_ref=batch_rows(count), dst_ref=batch_rows(count), send_sem=send_sem,
                recv_sem=recv_sem.at[level, part], device_id=seat_coords(target(1)), device_id_type=MESH,
            ).wait_recv()
            for spot, step in enumerate(steps):
                group, core = origin(step)
                lane = spot % 2
                part_sum = absorb(level, group * CORES + core, 1.0 - 2.0 * lane)
                totals[lane] = part_sum if totals[lane] is None else totals[lane] + part_sum
        total = totals[0] - totals[1]
        total = total[0:height] + total[height : 2 * height] + total[2 * height : 3 * height]
        sums_buf[my_core * depth + my_depth, level] = total[0 : 3 * SUBLANES]

        def send_sums(step, carry):
            sums_copy((my_depth + step) % depth, level).start()
            return carry

        lax.fori_loop(jnp.where(my_core == lead, 1, 0), depth, send_sums, 0)
        return carry

    lax.fori_loop(0, depth, gather_level, 0)
    batch = min(32, owner_ref.shape[0])

    def locate(step, carry):
        rows = pl.ds(pl.multiple_of(step * SUBLANES, SUBLANES), SUBLANES)
        source = source_ref[rows, :]
        lane, tile = source % LANES, source // LANES

        def look(group, found):
            for t in range(batch):
                row = group * batch + t
                entry = jnp.broadcast_to(owner_ref[pl.ds(row, 1), :], (SUBLANES, LANES))
                found = jnp.where(tile == row, gather_lanes(entry, lane), found)
            return found

        found = jnp.full((SUBLANES, LANES), -1, jnp.int32)
        if owner_ref.shape[0] == batch:
            found = look(0, found)
        else:
            found = lax.fori_loop(0, owner_ref.shape[0] // batch, look, found)
        place_buf[rows, :] = found % LANES
        return carry

    lax.fori_loop(0, source_ref.shape[0] // SUBLANES, locate, 0)


    at = {(0, 0): 0, (0, 1): 1, (0, 2): 2, (0, 3): 3, (0, 4): 4, (0, 5): 5, (5, 5): 6,
          (3, 5): 8, (1, 1): 9, (1, 2): 10, (1, 3): 11, (1, 4): 12, (1, 5): 13, (3, 3): 14, (3, 4): 15,
          (4, 4): 16, (4, 5): 17, (2, 2): 18, (2, 3): 19, (2, 4): 20, (2, 5): 21}

    senders = pl.ds(0, CORES * depth - 1)

    def fit_level(level, carry):
        pltpu.make_async_remote_copy(
            src_ref=sums_buf.at[senders, level, pl.ds(0, used)], dst_ref=sums_buf.at[senders, level, pl.ds(0, used)],
            send_sem=sums_send_sem, recv_sem=sums_recv_sem.at[level],
            device_id=level_coords((my_depth + 1) % depth), device_id_type=MESH,
        ).wait_recv()
        for core in range(CORES):
            fit(level, core)
        for step in range(plane - 1, 0, -1):
            table_copy(level, target(step)).start()
        return carry

    def fit(level, core):
        def gather_sums(slot, total):
            return total + sums_buf[core * depth + slot, level, 0:used, :]

        total = lax.fori_loop(1, depth, gather_sums, sums_buf[core * depth, level, 0:used, :], unroll=few)
        meta = meta_buf[core * depth + level]

        def entry(i, j):
            spot = at[min(i, j), max(i, j)]
            return total[spot : spot + 1, :]

        normal = [[entry(i, j) for j in range(params)] for i in range(params)]
        moments = [entry(i, params) for i in range(params)]
        with_prior = [[normal[i][j] for j in range(params)] for i in range(params)]
        for i in range(params):
            with_prior[i][i] = normal[i][i] + meta[i : i + 1, :]
        updates = solve_rows(with_prior, moments)
        squares = entry(params, params)
        for i in range(params):
            fitted = normal[i][0] * updates[0]
            for j in range(1, params):
                fitted = fitted + normal[i][j] * updates[j]
            squares = squares + updates[i] * (fitted - 2.0 * moments[i])
        minus = jnp.full((1, LANES), -1.0, jnp.float32)
        tables[my_group * members + level * CORES + core] = jnp.concatenate(
            updates + [minus, squares, meta[params:items, :]], axis=0
        )

    @pl.when(my_core == lead)
    def lead_fits():
        pltpu.make_async_remote_copy(
            src_ref=meta_buf.at[pl.ds(0, depth)], dst_ref=meta_buf.at[pl.ds(0, depth)],
            send_sem=meta_send_sem, recv_sem=meta_lead_sem, device_id=level_coords(my_depth, 0), device_id_type=MESH,
        ).wait_recv()
        lax.fori_loop(0, depth, fit_level, 0)


    def drain(ref, semaphore):
        pltpu.make_async_remote_copy(
            src_ref=ref, dst_ref=ref, send_sem=semaphore, recv_sem=meta_recv_sem,
            device_id=seat_coords(target(1)), device_id_type=MESH,
        ).wait_send()

    def refit_level(level, tails):
        def await_tables(count):
            pairs = pl.ds(0, count * CORES)
            pltpu.make_async_remote_copy(
                src_ref=tables.at[pairs], dst_ref=tables.at[pairs],
                send_sem=table_send_sem, recv_sem=table_recv_sem.at[level],
                device_id=seat_coords(target(1)), device_id_type=MESH,
            ).wait_recv()

        @pl.when(my_core == lead)
        def await_leads():
            await_tables(groups - 1)

        @pl.when(my_core != lead)
        def await_all():
            await_tables(groups)

        for seat in range(plane):
            k = seat // CORES * members + level * CORES + seat % CORES
            table = tables[k]
            tails = tails + table[items : words + 1, :]
            for piece in range(pieces):
                row = pl.ds(k * pieces + piece, 1)
                place = jnp.broadcast_to(place_buf[row, :], (SUBLANES, LANES))
                picked = gather_lanes(table, place)
                rows = out_buf[k, :, piece * LANES : (piece + 1) * LANES]
                fresh = -jnp.sum(jnp.where(sublane < items, picked * rows, 0.0), axis=0, keepdims=True)
                live = rows[words : words + 1, :] < picked[words : words + 1, :]
                root_buf[row, :] = jnp.where(live, fresh, 0.0)
        return tails

    tails = lax.fori_loop(0, depth - 1, refit_level, jnp.zeros((2, LANES), jnp.float32))
    sent = depth * (plane - 1)
    drain(out_buf.at[pl.ds(0, sent), pl.ds(0, words)], send_sem)

    @pl.when(my_core == lead)
    def drain_lead():
        drain(meta_buf.at[pl.ds(0, depth - 1)], meta_send_sem)
        drain(sums_buf.at[pl.ds(0, depth - 1), :, pl.ds(0, used)], sums_send_sem)

    @pl.when(my_core != lead)
    def drain_follower():
        drain(meta_buf.at[pl.ds(0, CORES * depth - 1)], meta_send_sem)
        drain(sums_buf.at[pl.ds(0, depth), :, pl.ds(0, used)], sums_send_sem)

    tails = refit_level(depth - 1, tails)
    tails = jnp.sum(tails, axis=1, keepdims=True)
    updates_ref[...] = tables[me, 0:params, :]
    norm = jnp.sqrt(jnp.maximum(tails[0:1], 0.0) / tails[1:2] + 1e-06)
    norm_ref[...] = jnp.broadcast_to(norm, norm_ref.shape)
    scale = 1.0 / norm
    fresh_ref[...] = root_buf[...] * scale

    @pl.when(my_core == lead)
    def drain_tables():
        def drain_seat(step, carry):
            drain(tables.at[pl.ds(0, depth * CORES)], table_send_sem)
            return carry

        lax.fori_loop(1, plane, drain_seat, 0)


def release(a_ref, b_ref, c_ref, a_out, b_out, c_out, sem):
    pairs = ((a_ref, a_out), (b_ref, b_out), (c_ref, c_out))
    copies = [pltpu.make_async_copy(x, y, sem.at[i]) for i, (x, y) in enumerate(pairs)]
    for copy in copies:
        copy.start()
    for copy in copies:
        copy.wait()


def body(source_id, slot, owner, counts, partials, residual, weight, prior):
    groups, members = lax.axis_size("grp"), lax.axis_size("dev")
    n = groups * members
    params = partials.shape[0]
    row_count = residual.shape[0]
    src_local = counts.shape[0]
    block_rows = row_count // n
    width = -(-block_rows // LANES) * LANES
    depth, plane = members // CORES, groups * CORES

    def lay(array, fill):
        if width == block_rows:
            return array
        blocks = array.reshape(-1, n, block_rows)
        blocks = jnp.pad(blocks, ((0, 0), (0, 0), (0, width - block_rows)), constant_values=fill)
        return blocks.reshape(array.shape[:-1] + (n * width,))

    def dense(array, fill):
        return lay(array, fill).reshape(-1, LANES)

    vmem = pl.BlockSpec(memory_space=pltpu.VMEM)
    operands = (
        dense(source_id, -1),
        dense(slot, 0),
        owner.reshape(-1, LANES),
        counts.reshape(1, src_local),
        lay(partials, 0),
        dense(residual, 0),
        dense(weight, 1),
        prior,
    )
    operands = tuple(pltpu.with_memory_space_constraint(x, pltpu.HBM) for x in operands)
    rows = n * width // LANES
    updates, standardized, norm = pl.pallas_call(
        functools.partial(kernel, (groups, members, width, row_count // src_local)),
        out_shape=(
            pltpu.VMEM((params, src_local), jnp.float32),
            pltpu.VMEM((rows, LANES), jnp.float32),
            pltpu.VMEM((1, LANES), jnp.float32),
        ),
        in_specs=[pl.BlockSpec(memory_space=pltpu.HBM)] * len(operands),
        out_specs=(vmem, vmem, vmem),
        scratch_shapes=[pltpu.VMEM(operand.shape, operand.dtype) for operand in operands] + [
            pltpu.VMEM((rows, LANES), jnp.float32),
            pltpu.VMEM((rows, LANES), jnp.float32),
            pltpu.VMEM((rows, LANES), jnp.int32),
            pltpu.VMEM((n, SUBLANES, width), jnp.float32),
            pltpu.VMEM((depth, plane, SUBLANES, width), jnp.float32),
            pltpu.VMEM((CORES * depth, SUBLANES, LANES), jnp.float32),
            pltpu.VMEM((depth, src_local, LANES), jnp.int32),
            pltpu.VMEM((depth, src_local, LANES), jnp.uint32),
            pltpu.VMEM((CORES * depth, depth, 3 * SUBLANES, LANES), jnp.float32),
            pltpu.VMEM((n, SUBLANES, LANES), jnp.float32),
            pltpu.SemaphoreType.DMA((len(operands),)),
            pltpu.SemaphoreType.DMA,
            pltpu.SemaphoreType.DMA((depth, 2)),
            pltpu.SemaphoreType.DMA,
            pltpu.SemaphoreType.DMA,
            pltpu.SemaphoreType.DMA,
            pltpu.SemaphoreType.DMA,
            pltpu.SemaphoreType.DMA((depth,)),
            pltpu.SemaphoreType.DMA,
            pltpu.SemaphoreType.DMA((depth,)),
        ],
        compiler_params=pltpu.CompilerParams(
            collective_id=0, has_side_effects=True, vmem_limit_bytes=40 << 20
        ),
        name="exchange_fit",
    )(*operands)
    results = (updates, standardized, norm)
    updates, standardized, norm = pl.pallas_call(
        release,
        out_shape=tuple(jax.ShapeDtypeStruct(r.shape, r.dtype) for r in results),
        in_specs=[vmem] * 3,
        out_specs=[pl.BlockSpec(memory_space=pltpu.HBM)] * 3,
        scratch_shapes=[pltpu.SemaphoreType.DMA((3,))],
        compiler_params=pltpu.CompilerParams(vmem_limit_bytes=4 << 20),
        name="release",
    )(*results)
    standardized = standardized.reshape(n, width)[:, :block_rows] if width != block_rows else standardized
    return (updates, standardized.reshape(row_count), norm[0, 0])


def solution(mesh):
    in_specs = (
        P(("grp", "dev")),
        P(("grp", "dev")),
        P(),
        P(("grp", "dev")),
        P(None, ("grp", "dev")),
        P(("grp", "dev")),
        P(("grp", "dev")),
        P(None, ("grp", "dev")),
    )
    out_specs = (P(None, ("grp", "dev")), P(("grp", "dev")), P())
    return jax.shard_map(body, mesh=mesh, in_specs=in_specs, out_specs=out_specs, check_vma=False)
```

```python
import functools

import jax
import jax.numpy as jnp
from jax import lax
from jax.experimental import pallas as pl
from jax.experimental.pallas import tpu as pltpu
from jax.sharding import PartitionSpec as P

LANES = 128
SUBLANES = 8
CORES = 2
MESH = pl.DeviceIdType.MESH


def solve_rows(normal, moments):
    params = len(moments)
    factor = {}
    inverse = []
    for column in range(params):
        running = normal[column][column]
        for earlier in range(column):
            running = running - factor[column, earlier] ** 2
        inverse.append(1.0 / jnp.sqrt(running))
        for target in range(column + 1, params):
            current = normal[target][column]
            for earlier in range(column):
                current = current - factor[target, earlier] * factor[column, earlier]
            factor[target, column] = current * inverse[column]
    forward = []
    for target in range(params):
        current = moments[target]
        for earlier in range(target):
            current = current - factor[target, earlier] * forward[earlier]
        forward.append(current * inverse[target])
    backward = [None] * params
    for target in reversed(range(params)):
        current = forward[target]
        for later in range(target + 1, params):
            current = current - factor[later, target] * backward[later]
        backward[target] = current * inverse[target]
    return backward


def thirds(values):
    high = values.astype(jnp.bfloat16)
    rest = values - high.astype(jnp.float32)
    middle = rest.astype(jnp.bfloat16)
    last = (rest - middle.astype(jnp.float32)).astype(jnp.bfloat16)
    return jnp.concatenate([high, middle, last], axis=0)


def gather_lanes(table, index):
    return jnp.take_along_axis(table, index, axis=1, mode="promise_in_bounds")


def kernel(
    sizes,
    source_hbm, slot_hbm, owner_hbm, counts_hbm, partials_hbm, residual_hbm, weight_hbm, prior_hbm,
    updates_ref, fresh_ref, norm_ref,
    source_ref, slot_ref, owner_ref, counts_ref, partials_ref, residual_ref, weight_ref, prior_ref,
    root_buf, cell_buf, place_buf, out_buf, in_buf, meta_buf, first_buf, room_buf, sums_buf, tables,
    load_sem, send_sem, recv_sem, meta_send_sem, meta_recv_sem, sums_send_sem, sums_recv_sem,
    table_send_sem, table_recv_sem,
):
    groups, members, width, pad_slots = sizes
    n = groups * members
    params = partials_ref.shape[0]
    words = params + 2
    items = params + 1
    depth = members // CORES
    plane = groups * CORES
    pieces = width // LANES
    low = 2 if groups % 2 == 0 else 1
    high = groups // low
    row_pairs = (
        (owner_hbm, owner_ref), (source_hbm, source_ref), (slot_hbm, slot_ref), (weight_hbm, weight_ref),
        (residual_hbm, residual_ref), (partials_hbm, partials_ref), (counts_hbm, counts_ref), (prior_hbm, prior_ref),
    )
    loads = [pltpu.make_async_copy(a, b, load_sem.at[i]) for i, (a, b) in enumerate(row_pairs)]
    for load in loads:
        load.start()
    my_group, my_member = lax.axis_index("grp"), lax.axis_index("dev")
    my_depth, my_core = my_member // CORES, my_member % CORES
    me = my_group * members + my_member
    my_seat = my_group * CORES + my_core

    def target(step):
        jump = step // CORES
        group = (my_group // low + jump // low) % high * low + (my_group % low + jump % low) % low
        return group, (my_core + step % CORES) % CORES

    def origin(step):
        jump = step // CORES
        group = (my_group // low + high - jump // low) % high * low + (my_group % low + low - jump % low) % low
        return group, (my_core + CORES - step % CORES) % CORES

    def seat_coords(seat):
        group, core = seat
        return (group, my_depth * CORES + core)

    def level_coords(level, core=None):
        return (my_group, level * CORES + (my_core if core is None else core))

    lead = CORES - 1

    def unit_of(index):
        return index // CORES * CORES + my_core, index % CORES

    def home_of(level, core):
        return level % CORES, level // CORES * CORES + core

    def far_first(step):
        return jnp.where(my_depth < depth // 2, depth - 1 - step, step)

    barrier = pltpu.get_barrier_semaphore()
    few = depth <= 4
    used = 3 * SUBLANES - 2

    def greet_level(step, carry):
        level = far_first(step)

        @pl.when(level != my_depth)
        def greet():
            for core in range(CORES):
                pl.semaphore_signal(barrier, inc=1, device_id=level_coords(level, core), device_id_type=MESH)

        return carry

    lax.fori_loop(0, depth, greet_level, 0, unroll=few)
    for step in range(plane - 1, 0, -1):
        pl.semaphore_signal(barrier, inc=1, device_id=seat_coords(target(step)), device_id_type=MESH)

    for load in loads:
        load.wait()

    meta_buf[my_core * depth + my_depth] = jnp.concatenate(
        [prior_ref[...], counts_ref[...].astype(jnp.float32), jnp.zeros((SUBLANES - items, LANES), jnp.float32)], axis=0
    )
    root = jnp.sqrt(weight_ref[...])
    root_buf[...] = root
    residual_ref[...] = residual_ref[...] * root
    cell_buf[...] = (source_ref[...] * pad_slots + slot_ref[...]).astype(jnp.float32)

    sublane = lax.broadcasted_iota(jnp.int32, (SUBLANES, LANES), 0)

    def prepare(level, seat, carry):
        k = seat // CORES * members + level * CORES + seat % CORES
        for piece in range(pieces):
            row = pl.ds(k * pieces + piece, 1)
            cols = pl.ds(pl.multiple_of(k * width + piece * LANES, LANES), LANES)

            def spread(ref):
                return jnp.broadcast_to(ref[row, :], (SUBLANES, LANES))

            scaled = partials_ref[:, cols] * jnp.broadcast_to(root_buf[row, :], (params, LANES))
            part = slice(piece * LANES, (piece + 1) * LANES)
            out_buf[k, 0:params, part] = scaled
            out_buf[k, params:items, part] = residual_ref[row, :]
            out_buf[k, items:words, part] = cell_buf[row, :]
            out_buf[k, words : words + 1, part] = slot_ref[row, :].astype(jnp.float32)
        return carry

    def prepare_level(level, carry):
        return lax.fori_loop(0, plane, functools.partial(prepare, level), carry, unroll=2)

    prepare_level(0, 0)

    pl.semaphore_wait(barrier, plane - 1 + CORES * (depth - 1))

    def meta_copy(level, core):
        slot = my_core * depth + my_depth
        return pltpu.make_async_remote_copy(
            src_ref=meta_buf.at[slot], dst_ref=meta_buf.at[slot], send_sem=meta_send_sem, recv_sem=meta_recv_sem,
            device_id=level_coords(level, core), device_id_type=MESH,
        )

    def row_copy(level, core, jump, part):
        home, unit = home_of(level, core)
        group, _ = target(jump * CORES)
        return pltpu.make_async_remote_copy(
            src_ref=out_buf.at[group * members + level * CORES + core, pl.ds(0, words)],
            dst_ref=in_buf.at[unit, my_seat, pl.ds(0, words)],
            send_sem=send_sem, recv_sem=recv_sem.at[unit, part],
            device_id=seat_coords((group, home)), device_id_type=MESH,
        )

    def sums_copy(level, stage, core):
        slot = core * depth + my_depth
        return pltpu.make_async_remote_copy(
            src_ref=sums_buf.at[slot, stage, pl.ds(0, used)], dst_ref=sums_buf.at[slot, stage, pl.ds(0, used)],
            send_sem=sums_send_sem, recv_sem=sums_recv_sem.at[stage],
            device_id=level_coords(level, lead), device_id_type=MESH,
        )

    def table_copy(stage, seat):
        pair = pl.ds(my_group * members + stage * CORES, CORES)
        return pltpu.make_async_remote_copy(
            src_ref=tables.at[pair], dst_ref=tables.at[pair],
            send_sem=table_send_sem, recv_sem=table_recv_sem.at[stage],
            device_id=seat_coords(seat), device_id_type=MESH,
        )

    def send_meta(step, carry):
        level = far_first(step)
        for core in range(CORES):
            pl.when(jnp.logical_or(level != my_depth, my_core != core))(meta_copy(level, core).start)
        return carry

    lax.fori_loop(0, depth, send_meta, 0, unroll=few)
    batches = ([0] + list(range(groups - 1, groups // 2, -1)), list(range(groups // 2, 0, -1)))

    def send_rows(level):
        for core in range(CORES):
            for jump in range(groups - 1, -1, -1):
                copy = row_copy(level, core, jump, int(jump in batches[1]))
                if jump:
                    copy.start()
                else:
                    pl.when(home_of(level, core)[0] != my_core)(copy.start)

    def stream_rows(level, carry):
        prepare_level(level, 0)
        send_rows(level - 1)
        return carry

    lax.fori_loop(1, depth, stream_rows, 0)
    send_rows(depth - 1)

    def own_rows(unit, carry):
        level, core = unit_of(unit)
        in_buf[unit, my_seat] = out_buf[my_group * members + level * CORES + core]
        return carry

    lax.fori_loop(0, depth, own_rows, 0)

    src_local = counts_ref.shape[1]
    square = (src_local, LANES)
    row_index = lax.broadcasted_iota(jnp.int32, square, 0)
    lane_index = lax.broadcasted_iota(jnp.int32, square, 1)
    diagonal = row_index == lane_index
    spare = 4

    def invert(unit, carry):
        level, core = unit_of(unit)
        position = (my_group * members + level * CORES + core) * src_local + row_index

        def scan(step, total):
            for part in range(spare):
                tile = step * spare + part
                total = jnp.where(owner_ref[pl.ds(tile, 1), :] == position, tile * LANES + lane_index, total)
            return total

        found = lax.fori_loop(0, owner_ref.shape[0] // spare, scan, jnp.zeros(square, jnp.int32))
        source_at = jnp.sum(found.astype(jnp.float32), axis=1, keepdims=True)
        first_buf[unit] = jnp.broadcast_to(source_at * pad_slots, square).astype(jnp.int32)
        return carry

    lax.fori_loop(0, depth, invert, 0)

    others = pl.ds(0, CORES * depth - 1)
    pltpu.make_async_remote_copy(
        src_ref=meta_buf.at[others], dst_ref=meta_buf.at[others], send_sem=meta_send_sem, recv_sem=meta_recv_sem,
        device_id=level_coords((my_depth + 1) % depth), device_id_type=MESH,
    ).wait_recv()

    def find_room(unit, carry):
        level, core = unit_of(unit)
        counts = meta_buf[core * depth + level, params:items, :]
        counts = jnp.sum(jnp.where(diagonal, counts, 0.0), axis=1, keepdims=True)
        room_buf[unit] = jnp.broadcast_to(counts, square).astype(jnp.int32).astype(jnp.uint32)
        return carry

    lax.fori_loop(0, depth, find_room, 0, unroll=few)
    wide_sublane = lax.broadcasted_iota(jnp.int32, (SUBLANES, width), 0)

    low_rows = wide_sublane < 2
    sixth_row = wide_sublane == items
    outer_rows = jnp.logical_or(wide_sublane == 0, wide_sublane >= items)

    def absorb(unit, slot, sign):
        first_cell, room = first_buf[unit], room_buf[unit]
        rows = in_buf[unit, slot]

        def spread(i):
            return jnp.broadcast_to(in_buf[unit, slot, i : i + 1, :], (SUBLANES, width))

        hot = []
        for piece in range(pieces):
            part = in_buf[unit, slot, items:words, piece * LANES : (piece + 1) * LANES].astype(jnp.int32)
            hit = (part - first_cell).astype(jnp.uint32) < room
            hot.append(jnp.where(hit, sign, 0.0))
        hot = jnp.concatenate(hot, axis=1).astype(jnp.bfloat16)
        products = jnp.concatenate(
            [
                jnp.where(sixth_row, spread(5), spread(0)) * jnp.where(sixth_row, pltpu.roll(rows, 1, 0), rows),
                jnp.where(outer_rows, spread(3), spread(1)) * jnp.where(outer_rows, pltpu.roll(rows, 3, 0), rows),
                jnp.where(low_rows, spread(4), spread(2)) * jnp.where(low_rows, pltpu.roll(rows, 4, 0), rows),
                jnp.zeros((SUBLANES, width), jnp.float32),
            ],
            axis=0,
        )
        return lax.dot_general(
            thirds(products), hot, (((1,), (1,)), ((), ())), preferred_element_type=jnp.float32
        )

    height = 4 * SUBLANES

    def gather_unit(unit, carry):
        level, owner_core = unit_of(unit)
        totals = [None, None]
        for part, jumps in enumerate(batches):
            count = CORES * len(jumps) - (part == 0)
            block = in_buf.at[unit, pl.ds(0, count), pl.ds(0, words)]
            pltpu.make_async_remote_copy(
                src_ref=block, dst_ref=block, send_sem=send_sem, recv_sem=recv_sem.at[unit, part],
                device_id=seat_coords(target(1)), device_id_type=MESH,
            ).wait_recv()
            for jump in jumps:
                group, _ = origin(jump * CORES)
                for core in range(CORES):
                    part_sum = absorb(unit, group * CORES + core, 1.0 - 2.0 * core)
                    totals[core] = part_sum if totals[core] is None else totals[core] + part_sum
        total = totals[0] - totals[1]
        total = total[0:height] + total[height : 2 * height] + total[2 * height : 3 * height]
        sums_buf[owner_core * depth + my_depth, level] = total[0 : 3 * SUBLANES]

        def send_sums(step, carry):
            aim = far_first(step)
            pl.when(jnp.logical_or(aim != my_depth, my_core != lead))(sums_copy(aim, level, owner_core).start)
            return carry

        lax.fori_loop(0, depth, send_sums, 0, unroll=few)
        return carry

    lax.fori_loop(0, depth, gather_unit, 0)
    batch = min(32, owner_ref.shape[0])

    def locate(step, carry):
        rows = pl.ds(pl.multiple_of(step * SUBLANES, SUBLANES), SUBLANES)
        source = source_ref[rows, :]
        lane, tile = source % LANES, source // LANES

        def look(group, found):
            for t in range(batch):
                row = group * batch + t
                entry = jnp.broadcast_to(owner_ref[pl.ds(row, 1), :], (SUBLANES, LANES))
                found = jnp.where(tile == row, gather_lanes(entry, lane), found)
            return found

        found = jnp.full((SUBLANES, LANES), -1, jnp.int32)
        if owner_ref.shape[0] == batch:
            found = look(0, found)
        else:
            found = lax.fori_loop(0, owner_ref.shape[0] // batch, look, found)
        place_buf[rows, :] = found % LANES
        return carry

    lax.fori_loop(0, source_ref.shape[0] // SUBLANES, locate, 0)


    at = {(0, 0): 0, (0, 1): 1, (0, 2): 2, (0, 3): 3, (0, 4): 4, (0, 5): 5, (5, 5): 6,
          (3, 5): 8, (1, 1): 9, (1, 2): 10, (1, 3): 11, (1, 4): 12, (1, 5): 13, (3, 3): 14, (3, 4): 15,
          (4, 4): 16, (4, 5): 17, (2, 2): 18, (2, 3): 19, (2, 4): 20, (2, 5): 21}

    def fit_level(level, count):
        block = sums_buf.at[pl.ds(0, count), level, pl.ds(0, used)]
        pltpu.make_async_remote_copy(
            src_ref=block, dst_ref=block, send_sem=sums_send_sem, recv_sem=sums_recv_sem.at[level],
            device_id=level_coords((my_depth + 1) % depth), device_id_type=MESH,
        ).wait_recv()
        for core in range(CORES):
            fit(level, core)
        for step in range(plane - 1, 0, -1):
            table_copy(level, target(step)).start()

    def fit(level, core):
        def gather_sums(slot, total):
            return total + sums_buf[core * depth + slot, level, 0:used, :]

        total = lax.fori_loop(1, depth, gather_sums, sums_buf[core * depth, level, 0:used, :], unroll=few)
        meta = meta_buf[core * depth + level]

        def entry(i, j):
            spot = at[min(i, j), max(i, j)]
            return total[spot : spot + 1, :]

        normal = [[entry(i, j) for j in range(params)] for i in range(params)]
        moments = [entry(i, params) for i in range(params)]
        with_prior = [[normal[i][j] for j in range(params)] for i in range(params)]
        for i in range(params):
            with_prior[i][i] = normal[i][i] + meta[i : i + 1, :]
        updates = solve_rows(with_prior, moments)
        squares = entry(params, params)
        for i in range(params):
            fitted = normal[i][0] * updates[0]
            for j in range(1, params):
                fitted = fitted + normal[i][j] * updates[j]
            squares = squares + updates[i] * (fitted - 2.0 * moments[i])
        minus = jnp.full((1, LANES), -1.0, jnp.float32)
        tables[my_group * members + level * CORES + core] = jnp.concatenate(
            updates + [minus, squares, meta[params:items, :]], axis=0
        )

    @pl.when(my_core == lead)
    def lead_fits():
        def fit_pair(step, carry):
            for core in range(CORES):
                fit_level(step * CORES + core, CORES * (depth - (core == lead)))
            return carry

        lax.fori_loop(0, depth // CORES, fit_pair, 0)

    def drain(ref, semaphore):
        pltpu.make_async_remote_copy(
            src_ref=ref, dst_ref=ref, send_sem=semaphore, recv_sem=meta_recv_sem,
            device_id=seat_coords(target(1)), device_id_type=MESH,
        ).wait_send()

    def refit_level(level, tails):
        def await_tables(count):
            pairs = pl.ds(0, count * CORES)
            pltpu.make_async_remote_copy(
                src_ref=tables.at[pairs], dst_ref=tables.at[pairs],
                send_sem=table_send_sem, recv_sem=table_recv_sem.at[level],
                device_id=seat_coords(target(1)), device_id_type=MESH,
            ).wait_recv()

        @pl.when(my_core == lead)
        def await_leads():
            await_tables(groups - 1)

        @pl.when(my_core != lead)
        def await_all():
            await_tables(groups)

        for seat in range(plane):
            k = seat // CORES * members + level * CORES + seat % CORES
            table = tables[k]
            tails = tails + table[items : words + 1, :]
            for piece in range(pieces):
                row = pl.ds(k * pieces + piece, 1)
                place = jnp.broadcast_to(place_buf[row, :], (SUBLANES, LANES))
                picked = gather_lanes(table, place)
                rows = out_buf[k, :, piece * LANES : (piece + 1) * LANES]
                fresh = -jnp.sum(jnp.where(sublane < items, picked * rows, 0.0), axis=0, keepdims=True)
                live = rows[words : words + 1, :] < picked[words : words + 1, :]
                root_buf[row, :] = jnp.where(live, fresh, 0.0)
        return tails

    tails = lax.fori_loop(0, depth - 1, refit_level, jnp.zeros((2, LANES), jnp.float32))
    sent = depth * (plane - 1)
    drain(out_buf.at[pl.ds(0, sent), pl.ds(0, words)], send_sem)
    drain(meta_buf.at[others], meta_send_sem)

    @pl.when(my_core == lead)
    def drain_lead():
        drain(sums_buf.at[pl.ds(0, depth - 1), :, pl.ds(0, used)], sums_send_sem)

    @pl.when(my_core != lead)
    def drain_follower():
        drain(sums_buf.at[pl.ds(0, depth), :, pl.ds(0, used)], sums_send_sem)

    tails = refit_level(depth - 1, tails)
    tails = jnp.sum(tails, axis=1, keepdims=True)
    updates_ref[...] = tables[me, 0:params, :]
    norm = jnp.sqrt(jnp.maximum(tails[0:1], 0.0) / tails[1:2] + 1e-06)
    norm_ref[...] = jnp.broadcast_to(norm, norm_ref.shape)
    scale = 1.0 / norm
    fresh_ref[...] = root_buf[...] * scale

    @pl.when(my_core == lead)
    def drain_tables():
        def drain_seat(step, carry):
            drain(tables.at[pl.ds(0, depth * CORES)], table_send_sem)
            return carry

        lax.fori_loop(1, plane, drain_seat, 0)


def release(a_ref, b_ref, c_ref, a_out, b_out, c_out, sem):
    pairs = ((a_ref, a_out), (b_ref, b_out), (c_ref, c_out))
    copies = [pltpu.make_async_copy(x, y, sem.at[i]) for i, (x, y) in enumerate(pairs)]
    for copy in copies:
        copy.start()
    for copy in copies:
        copy.wait()


def body(source_id, slot, owner, counts, partials, residual, weight, prior):
    groups, members = lax.axis_size("grp"), lax.axis_size("dev")
    n = groups * members
    params = partials.shape[0]
    row_count = residual.shape[0]
    src_local = counts.shape[0]
    block_rows = row_count // n
    width = -(-block_rows // LANES) * LANES
    depth, plane = members // CORES, groups * CORES

    def lay(array, fill):
        if width == block_rows:
            return array
        blocks = array.reshape(-1, n, block_rows)
        blocks = jnp.pad(blocks, ((0, 0), (0, 0), (0, width - block_rows)), constant_values=fill)
        return blocks.reshape(array.shape[:-1] + (n * width,))

    def dense(array, fill):
        return lay(array, fill).reshape(-1, LANES)

    vmem = pl.BlockSpec(memory_space=pltpu.VMEM)
    operands = (
        dense(source_id, -1),
        dense(slot, 0),
        owner.reshape(-1, LANES),
        counts.reshape(1, src_local),
        lay(partials, 0),
        dense(residual, 0),
        dense(weight, 1),
        prior,
    )
    operands = tuple(pltpu.with_memory_space_constraint(x, pltpu.HBM) for x in operands)
    rows = n * width // LANES
    updates, standardized, norm = pl.pallas_call(
        functools.partial(kernel, (groups, members, width, row_count // src_local)),
        out_shape=(
            pltpu.VMEM((params, src_local), jnp.float32),
            pltpu.VMEM((rows, LANES), jnp.float32),
            pltpu.VMEM((1, LANES), jnp.float32),
        ),
        in_specs=[pl.BlockSpec(memory_space=pltpu.HBM)] * len(operands),
        out_specs=(vmem, vmem, vmem),
        scratch_shapes=[pltpu.VMEM(operand.shape, operand.dtype) for operand in operands] + [
            pltpu.VMEM((rows, LANES), jnp.float32),
            pltpu.VMEM((rows, LANES), jnp.float32),
            pltpu.VMEM((rows, LANES), jnp.int32),
            pltpu.VMEM((n, SUBLANES, width), jnp.float32),
            pltpu.VMEM((depth, plane, SUBLANES, width), jnp.float32),
            pltpu.VMEM((CORES * depth, SUBLANES, LANES), jnp.float32),
            pltpu.VMEM((depth, src_local, LANES), jnp.int32),
            pltpu.VMEM((depth, src_local, LANES), jnp.uint32),
            pltpu.VMEM((CORES * depth, depth, 3 * SUBLANES, LANES), jnp.float32),
            pltpu.VMEM((n, SUBLANES, LANES), jnp.float32),
            pltpu.SemaphoreType.DMA((len(operands),)),
            pltpu.SemaphoreType.DMA,
            pltpu.SemaphoreType.DMA((depth, 2)),
            pltpu.SemaphoreType.DMA,
            pltpu.SemaphoreType.DMA,
            pltpu.SemaphoreType.DMA,
            pltpu.SemaphoreType.DMA((depth,)),
            pltpu.SemaphoreType.DMA,
            pltpu.SemaphoreType.DMA((depth,)),
        ],
        compiler_params=pltpu.CompilerParams(
            collective_id=0, has_side_effects=True, vmem_limit_bytes=40 << 20
        ),
        name="exchange_fit",
    )(*operands)
    results = (updates, standardized, norm)
    updates, standardized, norm = pl.pallas_call(
        release,
        out_shape=tuple(jax.ShapeDtypeStruct(r.shape, r.dtype) for r in results),
        in_specs=[vmem] * 3,
        out_specs=[pl.BlockSpec(memory_space=pltpu.HBM)] * 3,
        scratch_shapes=[pltpu.SemaphoreType.DMA((3,))],
        compiler_params=pltpu.CompilerParams(vmem_limit_bytes=4 << 20),
        name="release",
    )(*results)
    standardized = standardized.reshape(n, width)[:, :block_rows] if width != block_rows else standardized
    return (updates, standardized.reshape(row_count), norm[0, 0])


def solution(mesh):
    in_specs = (
        P(("grp", "dev")),
        P(("grp", "dev")),
        P(),
        P(("grp", "dev")),
        P(None, ("grp", "dev")),
        P(("grp", "dev")),
        P(("grp", "dev")),
        P(None, ("grp", "dev")),
    )
    out_specs = (P(None, ("grp", "dev")), P(("grp", "dev")), P())
    return jax.shard_map(body, mesh=mesh, in_specs=in_specs, out_specs=out_specs, check_vma=False)
```

```python
import functools

import jax
import jax.numpy as jnp
from jax import lax
from jax.experimental import pallas as pl
from jax.experimental.pallas import tpu as pltpu
from jax.sharding import PartitionSpec as P

LANES = 128
SUBLANES = 8
CORES = 2
MESH = pl.DeviceIdType.MESH


def solve_rows(normal, moments):
    params = len(moments)
    factor = {}
    inverse = []
    for column in range(params):
        running = normal[column][column]
        for earlier in range(column):
            running = running - factor[column, earlier] ** 2
        inverse.append(1.0 / jnp.sqrt(running))
        for target in range(column + 1, params):
            current = normal[target][column]
            for earlier in range(column):
                current = current - factor[target, earlier] * factor[column, earlier]
            factor[target, column] = current * inverse[column]
    forward = []
    for target in range(params):
        current = moments[target]
        for earlier in range(target):
            current = current - factor[target, earlier] * forward[earlier]
        forward.append(current * inverse[target])
    backward = [None] * params
    for target in reversed(range(params)):
        current = forward[target]
        for later in range(target + 1, params):
            current = current - factor[later, target] * backward[later]
        backward[target] = current * inverse[target]
    return backward


def thirds(values):
    high = values.astype(jnp.bfloat16)
    rest = values - high.astype(jnp.float32)
    middle = rest.astype(jnp.bfloat16)
    last = (rest - middle.astype(jnp.float32)).astype(jnp.bfloat16)
    return jnp.concatenate([high, middle, last], axis=0)


def gather_lanes(table, index):
    return jnp.take_along_axis(table, index, axis=1, mode="promise_in_bounds")


def kernel(
    sizes,
    source_hbm, slot_hbm, owner_hbm, counts_hbm, partials_hbm, residual_hbm, weight_hbm, prior_hbm,
    updates_ref, fresh_ref, norm_ref,
    source_ref, slot_ref, owner_ref, counts_ref, partials_ref, residual_ref, weight_ref, prior_ref,
    root_buf, cell_buf, place_buf, out_buf, in_buf, meta_buf, first_buf, room_buf, sums_buf, tables,
    load_sem, send_sem, recv_sem, meta_send_sem, meta_recv_sem, sums_send_sem, sums_recv_sem,
    table_send_sem, table_recv_sem, gate_sem,
):
    groups, members, width, pad_slots = sizes
    n = groups * members
    params = partials_ref.shape[0]
    words = params + 2
    items = params + 1
    depth = members // CORES
    plane = groups * CORES
    pieces = width // LANES
    low = 2 if groups % 2 == 0 else 1
    high = groups // low
    row_pairs = (
        (owner_hbm, owner_ref), (source_hbm, source_ref), (slot_hbm, slot_ref), (weight_hbm, weight_ref),
        (residual_hbm, residual_ref), (partials_hbm, partials_ref), (counts_hbm, counts_ref), (prior_hbm, prior_ref),
    )
    loads = [pltpu.make_async_copy(a, b, load_sem.at[i]) for i, (a, b) in enumerate(row_pairs)]
    for load in loads:
        load.start()
    my_group, my_member = lax.axis_index("grp"), lax.axis_index("dev")
    my_depth, my_core = my_member // CORES, my_member % CORES
    me = my_group * members + my_member
    my_seat = my_group * CORES + my_core

    def target(step):
        jump = step // CORES
        group = (my_group // low + jump // low) % high * low + (my_group % low + jump % low) % low
        return group, (my_core + step % CORES) % CORES

    def origin(step):
        jump = step // CORES
        group = (my_group // low + high - jump // low) % high * low + (my_group % low + low - jump % low) % low
        return group, (my_core + CORES - step % CORES) % CORES

    def seat_coords(seat):
        group, core = seat
        return (group, my_depth * CORES + core)

    def level_coords(level, core=None):
        return (my_group, level * CORES + (my_core if core is None else core))

    lead = CORES - 1

    def level_at(turn):
        return depth - 1 - turn

    def unit_of(index):
        return level_at(index // CORES * CORES + my_core), index % CORES

    def home_of(level, core):
        turn = depth - 1 - level
        return turn % CORES, turn // CORES * CORES + core

    def far_first(step):
        return jnp.where(my_depth < depth // 2, depth - 1 - step, step)

    barrier = pltpu.get_barrier_semaphore()
    few = depth <= 4
    used = 3 * SUBLANES - 2

    def tell(semaphore, level):
        for core in range(CORES):
            pl.semaphore_signal(semaphore, inc=1, device_id=level_coords(level, core), device_id_type=MESH)

    def greet_level(step, carry):
        level = level_at(step)
        pl.when(level > my_depth)(lambda: tell(barrier, level))
        return carry

    for step in range(plane - 1, 0, -1):
        pl.semaphore_signal(barrier, inc=1, device_id=seat_coords(target(step)), device_id_type=MESH)
    lax.fori_loop(0, depth, greet_level, 0, unroll=few)

    for load in loads:
        load.wait()

    meta_buf[my_core * depth + my_depth] = jnp.concatenate(
        [prior_ref[...], counts_ref[...].astype(jnp.float32), jnp.zeros((SUBLANES - items, LANES), jnp.float32)], axis=0
    )
    root = jnp.sqrt(weight_ref[...])
    root_buf[...] = root
    residual_ref[...] = residual_ref[...] * root
    cell_buf[...] = (source_ref[...] * pad_slots + slot_ref[...]).astype(jnp.float32)

    sublane = lax.broadcasted_iota(jnp.int32, (SUBLANES, LANES), 0)

    def prepare(level, seat, carry):
        k = seat // CORES * members + level * CORES + seat % CORES
        for piece in range(pieces):
            row = pl.ds(k * pieces + piece, 1)
            cols = pl.ds(pl.multiple_of(k * width + piece * LANES, LANES), LANES)

            def spread(ref):
                return jnp.broadcast_to(ref[row, :], (SUBLANES, LANES))

            scaled = partials_ref[:, cols] * jnp.broadcast_to(root_buf[row, :], (params, LANES))
            part = slice(piece * LANES, (piece + 1) * LANES)
            out_buf[k, 0:params, part] = scaled
            out_buf[k, params:items, part] = residual_ref[row, :]
            out_buf[k, items:words, part] = cell_buf[row, :]
            out_buf[k, words : words + 1, part] = slot_ref[row, :].astype(jnp.float32)
        return carry

    def prepare_level(level, carry):
        return lax.fori_loop(0, plane, functools.partial(prepare, level), carry, unroll=2)

    prepare_level(level_at(0), 0)

    pl.semaphore_wait(barrier, plane - 1 + CORES * my_depth)

    def meta_copy(level, core):
        slot = my_core * depth + my_depth
        return pltpu.make_async_remote_copy(
            src_ref=meta_buf.at[slot], dst_ref=meta_buf.at[slot], send_sem=meta_send_sem,
            recv_sem=meta_recv_sem.at[my_depth], device_id=level_coords(level, core), device_id_type=MESH,
        )

    def row_copy(level, core, jump, part):
        home, unit = home_of(level, core)
        group, _ = target(jump * CORES)
        return pltpu.make_async_remote_copy(
            src_ref=out_buf.at[group * members + level * CORES + core, pl.ds(0, words)],
            dst_ref=in_buf.at[unit, my_seat, pl.ds(0, words)],
            send_sem=send_sem, recv_sem=recv_sem.at[unit, part],
            device_id=seat_coords((group, home)), device_id_type=MESH,
        )

    def sums_copy(level, stage, core):
        slot = core * depth + my_depth
        return pltpu.make_async_remote_copy(
            src_ref=sums_buf.at[slot, stage, pl.ds(0, used)], dst_ref=sums_buf.at[slot, stage, pl.ds(0, used)],
            send_sem=sums_send_sem, recv_sem=sums_recv_sem.at[stage],
            device_id=level_coords(level, lead), device_id_type=MESH,
        )

    def table_copy(stage, seat):
        pair = pl.ds(my_group * members + stage * CORES, CORES)
        return pltpu.make_async_remote_copy(
            src_ref=tables.at[pair], dst_ref=tables.at[pair],
            send_sem=table_send_sem, recv_sem=table_recv_sem.at[stage],
            device_id=seat_coords(seat), device_id_type=MESH,
        )

    def send_meta_down(level, carry):
        for core in range(CORES):
            remote = jnp.logical_or(level < my_depth, jnp.logical_and(level == my_depth, my_core != core))
            pl.when(remote)(meta_copy(level, core).start)
        pl.when(level < my_depth)(lambda: tell(gate_sem, level))
        return carry

    def send_meta_up(step, carry):
        level = level_at(step)
        for core in range(CORES):
            pl.when(level > my_depth)(meta_copy(level, core).start)
        return carry

    lax.fori_loop(0, depth, send_meta_down, 0, unroll=few)
    batches = ([0] + list(range(groups - 1, groups // 2, -1)), list(range(groups // 2, 0, -1)))

    def send_rows(level):
        for core in range(CORES):
            for jump in range(groups - 1, -1, -1):
                copy = row_copy(level, core, jump, int(jump in batches[1]))
                if jump:
                    copy.start()
                else:
                    pl.when(home_of(level, core)[0] != my_core)(copy.start)

    def stream_rows(turn, carry):
        prepare_level(level_at(turn), 0)
        send_rows(level_at(turn - 1))
        return carry

    lax.fori_loop(1, depth, stream_rows, 0)
    send_rows(level_at(depth - 1))

    def own_rows(unit, carry):
        level, core = unit_of(unit)
        in_buf[unit, my_seat] = out_buf[my_group * members + level * CORES + core]
        return carry

    lax.fori_loop(0, depth, own_rows, 0)

    src_local = counts_ref.shape[1]
    square = (src_local, LANES)
    row_index = lax.broadcasted_iota(jnp.int32, square, 0)
    lane_index = lax.broadcasted_iota(jnp.int32, square, 1)
    diagonal = row_index == lane_index
    spare = 4

    def invert(unit, carry):
        level, core = unit_of(unit)
        position = (my_group * members + level * CORES + core) * src_local + row_index

        def scan(step, total):
            for part in range(spare):
                tile = step * spare + part
                total = jnp.where(owner_ref[pl.ds(tile, 1), :] == position, tile * LANES + lane_index, total)
            return total

        found = lax.fori_loop(0, owner_ref.shape[0] // spare, scan, jnp.zeros(square, jnp.int32))
        source_at = jnp.sum(found.astype(jnp.float32), axis=1, keepdims=True)
        first_buf[unit] = jnp.broadcast_to(source_at * pad_slots, square).astype(jnp.int32)
        return carry

    lax.fori_loop(0, depth, invert, 0)

    @pl.when(my_depth < depth - 1)
    def open_up():
        pl.semaphore_wait(gate_sem, CORES * (depth - 1 - my_depth))
        lax.fori_loop(0, depth, send_meta_up, 0, unroll=few)

    batch = min(32, owner_ref.shape[0])

    def locate(step, carry):
        rows = pl.ds(pl.multiple_of(step * SUBLANES, SUBLANES), SUBLANES)
        source = source_ref[rows, :]
        lane, tile = source % LANES, source // LANES

        def look(group, found):
            for t in range(batch):
                row = group * batch + t
                entry = jnp.broadcast_to(owner_ref[pl.ds(row, 1), :], (SUBLANES, LANES))
                found = jnp.where(tile == row, gather_lanes(entry, lane), found)
            return found

        found = jnp.full((SUBLANES, LANES), -1, jnp.int32)
        if owner_ref.shape[0] == batch:
            found = look(0, found)
        else:
            found = lax.fori_loop(0, owner_ref.shape[0] // batch, look, found)
        place_buf[rows, :] = found % LANES
        return carry

    lax.fori_loop(0, source_ref.shape[0] // SUBLANES, locate, 0)


    others = pl.ds(0, CORES * depth - 1)

    def await_meta(level):
        def take(count):
            block = meta_buf.at[pl.ds(0, count)]
            pltpu.make_async_remote_copy(
                src_ref=block, dst_ref=block, send_sem=meta_send_sem, recv_sem=meta_recv_sem.at[level],
                device_id=seat_coords(target(1)), device_id_type=MESH,
            ).wait_recv()

        pl.when(level == my_depth)(lambda: take(CORES - 1))
        pl.when(level != my_depth)(lambda: take(CORES))

    def find_room(unit, carry):
        level, core = unit_of(unit)
        counts = meta_buf[core * depth + level, params:items, :]
        counts = jnp.sum(jnp.where(diagonal, counts, 0.0), axis=1, keepdims=True)
        room_buf[unit] = jnp.broadcast_to(counts, square).astype(jnp.int32).astype(jnp.uint32)
        return carry

    wide_sublane = lax.broadcasted_iota(jnp.int32, (SUBLANES, width), 0)

    low_rows = wide_sublane < 2
    sixth_row = wide_sublane == items
    outer_rows = jnp.logical_or(wide_sublane == 0, wide_sublane >= items)

    def absorb(unit, slot, sign):
        first_cell, room = first_buf[unit], room_buf[unit]
        rows = in_buf[unit, slot]

        def spread(i):
            return jnp.broadcast_to(in_buf[unit, slot, i : i + 1, :], (SUBLANES, width))

        hot = []
        for piece in range(pieces):
            part = in_buf[unit, slot, items:words, piece * LANES : (piece + 1) * LANES].astype(jnp.int32)
            hit = (part - first_cell).astype(jnp.uint32) < room
            hot.append(jnp.where(hit, sign, 0.0))
        hot = jnp.concatenate(hot, axis=1).astype(jnp.bfloat16)
        products = jnp.concatenate(
            [
                jnp.where(sixth_row, spread(5), spread(0)) * jnp.where(sixth_row, pltpu.roll(rows, 1, 0), rows),
                jnp.where(outer_rows, spread(3), spread(1)) * jnp.where(outer_rows, pltpu.roll(rows, 3, 0), rows),
                jnp.where(low_rows, spread(4), spread(2)) * jnp.where(low_rows, pltpu.roll(rows, 4, 0), rows),
                jnp.zeros((SUBLANES, width), jnp.float32),
            ],
            axis=0,
        )
        return lax.dot_general(
            thirds(products), hot, (((1,), (1,)), ((), ())), preferred_element_type=jnp.float32
        )

    height = 4 * SUBLANES

    def gather_unit(unit, carry):
        level, owner_core = unit_of(unit)
        totals = [None, None]
        for part, jumps in enumerate(batches):
            count = CORES * len(jumps) - (part == 0)
            block = in_buf.at[unit, pl.ds(0, count), pl.ds(0, words)]
            pltpu.make_async_remote_copy(
                src_ref=block, dst_ref=block, send_sem=send_sem, recv_sem=recv_sem.at[unit, part],
                device_id=seat_coords(target(1)), device_id_type=MESH,
            ).wait_recv()
            for jump in jumps:
                group, _ = origin(jump * CORES)
                for core in range(CORES):
                    part_sum = absorb(unit, group * CORES + core, 1.0 - 2.0 * core)
                    totals[core] = part_sum if totals[core] is None else totals[core] + part_sum
        total = totals[0] - totals[1]
        total = total[0:height] + total[height : 2 * height] + total[2 * height : 3 * height]
        sums_buf[owner_core * depth + my_depth, level] = total[0 : 3 * SUBLANES]

        def send_sums(step, carry):
            aim = far_first(step)
            pl.when(jnp.logical_or(aim != my_depth, my_core != lead))(sums_copy(aim, level, owner_core).start)
            return carry

        lax.fori_loop(0, depth, send_sums, 0, unroll=few)
        return carry

    def gather_turn(turn, carry):
        await_meta(unit_of(turn * CORES)[0])
        lax.fori_loop(turn * CORES, (turn + 1) * CORES, find_room, 0)
        return lax.fori_loop(turn * CORES, (turn + 1) * CORES, gather_unit, carry)

    def other_meta(turn, carry):
        await_meta(level_at(turn * CORES + 1 - my_core))
        return carry

    lax.fori_loop(0, depth // CORES, gather_turn, 0)
    lax.fori_loop(0, depth // CORES, other_meta, 0)
    at = {(0, 0): 0, (0, 1): 1, (0, 2): 2, (0, 3): 3, (0, 4): 4, (0, 5): 5, (5, 5): 6,
          (3, 5): 8, (1, 1): 9, (1, 2): 10, (1, 3): 11, (1, 4): 12, (1, 5): 13, (3, 3): 14, (3, 4): 15,
          (4, 4): 16, (4, 5): 17, (2, 2): 18, (2, 3): 19, (2, 4): 20, (2, 5): 21}

    def fit_level(level, count):
        block = sums_buf.at[pl.ds(0, count), level, pl.ds(0, used)]
        pltpu.make_async_remote_copy(
            src_ref=block, dst_ref=block, send_sem=sums_send_sem, recv_sem=sums_recv_sem.at[level],
            device_id=level_coords((my_depth + 1) % depth), device_id_type=MESH,
        ).wait_recv()
        for core in range(CORES):
            fit(level, core)
        for step in range(plane - 1, 0, -1):
            table_copy(level, target(step)).start()

    def fit(level, core):
        def gather_sums(slot, total):
            return total + sums_buf[core * depth + slot, level, 0:used, :]

        total = lax.fori_loop(1, depth, gather_sums, sums_buf[core * depth, level, 0:used, :], unroll=few)
        meta = meta_buf[core * depth + level]

        def entry(i, j):
            spot = at[min(i, j), max(i, j)]
            return total[spot : spot + 1, :]

        normal = [[entry(i, j) for j in range(params)] for i in range(params)]
        moments = [entry(i, params) for i in range(params)]
        with_prior = [[normal[i][j] for j in range(params)] for i in range(params)]
        for i in range(params):
            with_prior[i][i] = normal[i][i] + meta[i : i + 1, :]
        updates = solve_rows(with_prior, moments)
        squares = entry(params, params)
        for i in range(params):
            fitted = normal[i][0] * updates[0]
            for j in range(1, params):
                fitted = fitted + normal[i][j] * updates[j]
            squares = squares + updates[i] * (fitted - 2.0 * moments[i])
        minus = jnp.full((1, LANES), -1.0, jnp.float32)
        tables[my_group * members + level * CORES + core] = jnp.concatenate(
            updates + [minus, squares, meta[params:items, :]], axis=0
        )

    @pl.when(my_core == lead)
    def lead_fits():
        def fit_pair(step, carry):
            for core in range(CORES):
                fit_level(level_at(step * CORES + core), CORES * (depth - (core == lead)))
            return carry

        lax.fori_loop(0, depth // CORES, fit_pair, 0)

    def drain(ref, semaphore):
        pltpu.make_async_remote_copy(
            src_ref=ref, dst_ref=ref, send_sem=semaphore, recv_sem=meta_recv_sem.at[0],
            device_id=seat_coords(target(1)), device_id_type=MESH,
        ).wait_send()

    def refit_level(turn, tails):
        level = level_at(turn)

        def await_tables(count):
            pairs = pl.ds(0, count * CORES)
            pltpu.make_async_remote_copy(
                src_ref=tables.at[pairs], dst_ref=tables.at[pairs],
                send_sem=table_send_sem, recv_sem=table_recv_sem.at[level],
                device_id=seat_coords(target(1)), device_id_type=MESH,
            ).wait_recv()

        @pl.when(my_core == lead)
        def await_leads():
            await_tables(groups - 1)

        @pl.when(my_core != lead)
        def await_all():
            await_tables(groups)

        for seat in range(plane):
            k = seat // CORES * members + level * CORES + seat % CORES
            table = tables[k]
            tails = tails + table[items : words + 1, :]
            for piece in range(pieces):
                row = pl.ds(k * pieces + piece, 1)
                place = jnp.broadcast_to(place_buf[row, :], (SUBLANES, LANES))
                picked = gather_lanes(table, place)
                rows = out_buf[k, :, piece * LANES : (piece + 1) * LANES]
                fresh = -jnp.sum(jnp.where(sublane < items, picked * rows, 0.0), axis=0, keepdims=True)
                live = rows[words : words + 1, :] < picked[words : words + 1, :]
                root_buf[row, :] = jnp.where(live, fresh, 0.0)
        return tails

    tails = lax.fori_loop(0, depth - 1, refit_level, jnp.zeros((2, LANES), jnp.float32))
    sent = depth * (plane - 1)
    drain(out_buf.at[pl.ds(0, sent), pl.ds(0, words)], send_sem)
    drain(meta_buf.at[others], meta_send_sem)

    @pl.when(my_core == lead)
    def drain_lead():
        drain(sums_buf.at[pl.ds(0, depth - 1), :, pl.ds(0, used)], sums_send_sem)

    @pl.when(my_core != lead)
    def drain_follower():
        drain(sums_buf.at[pl.ds(0, depth), :, pl.ds(0, used)], sums_send_sem)

    tails = refit_level(depth - 1, tails)
    tails = jnp.sum(tails, axis=1, keepdims=True)
    updates_ref[...] = tables[me, 0:params, :]
    norm = jnp.sqrt(jnp.maximum(tails[0:1], 0.0) / tails[1:2] + 1e-06)
    norm_ref[...] = jnp.broadcast_to(norm, norm_ref.shape)
    scale = 1.0 / norm
    fresh_ref[...] = root_buf[...] * scale

    @pl.when(my_core == lead)
    def drain_tables():
        def drain_seat(step, carry):
            drain(tables.at[pl.ds(0, depth * CORES)], table_send_sem)
            return carry

        lax.fori_loop(1, plane, drain_seat, 0)


def release(a_ref, b_ref, c_ref, a_out, b_out, c_out, sem):
    pairs = ((a_ref, a_out), (b_ref, b_out), (c_ref, c_out))
    copies = [pltpu.make_async_copy(x, y, sem.at[i]) for i, (x, y) in enumerate(pairs)]
    for copy in copies:
        copy.start()
    for copy in copies:
        copy.wait()


def body(source_id, slot, owner, counts, partials, residual, weight, prior):
    groups, members = lax.axis_size("grp"), lax.axis_size("dev")
    n = groups * members
    params = partials.shape[0]
    row_count = residual.shape[0]
    src_local = counts.shape[0]
    block_rows = row_count // n
    width = -(-block_rows // LANES) * LANES
    depth, plane = members // CORES, groups * CORES

    def lay(array, fill):
        if width == block_rows:
            return array
        blocks = array.reshape(-1, n, block_rows)
        blocks = jnp.pad(blocks, ((0, 0), (0, 0), (0, width - block_rows)), constant_values=fill)
        return blocks.reshape(array.shape[:-1] + (n * width,))

    def dense(array, fill):
        return lay(array, fill).reshape(-1, LANES)

    vmem = pl.BlockSpec(memory_space=pltpu.VMEM)
    operands = (
        dense(source_id, -1),
        dense(slot, 0),
        owner.reshape(-1, LANES),
        counts.reshape(1, src_local),
        lay(partials, 0),
        dense(residual, 0),
        dense(weight, 1),
        prior,
    )
    operands = tuple(pltpu.with_memory_space_constraint(x, pltpu.HBM) for x in operands)
    rows = n * width // LANES
    updates, standardized, norm = pl.pallas_call(
        functools.partial(kernel, (groups, members, width, row_count // src_local)),
        out_shape=(
            pltpu.VMEM((params, src_local), jnp.float32),
            pltpu.VMEM((rows, LANES), jnp.float32),
            pltpu.VMEM((1, LANES), jnp.float32),
        ),
        in_specs=[pl.BlockSpec(memory_space=pltpu.HBM)] * len(operands),
        out_specs=(vmem, vmem, vmem),
        scratch_shapes=[pltpu.VMEM(operand.shape, operand.dtype) for operand in operands] + [
            pltpu.VMEM((rows, LANES), jnp.float32),
            pltpu.VMEM((rows, LANES), jnp.float32),
            pltpu.VMEM((rows, LANES), jnp.int32),
            pltpu.VMEM((n, SUBLANES, width), jnp.float32),
            pltpu.VMEM((depth, plane, SUBLANES, width), jnp.float32),
            pltpu.VMEM((CORES * depth, SUBLANES, LANES), jnp.float32),
            pltpu.VMEM((depth, src_local, LANES), jnp.int32),
            pltpu.VMEM((depth, src_local, LANES), jnp.uint32),
            pltpu.VMEM((CORES * depth, depth, 3 * SUBLANES, LANES), jnp.float32),
            pltpu.VMEM((n, SUBLANES, LANES), jnp.float32),
            pltpu.SemaphoreType.DMA((len(operands),)),
            pltpu.SemaphoreType.DMA,
            pltpu.SemaphoreType.DMA((depth, 2)),
            pltpu.SemaphoreType.DMA,
            pltpu.SemaphoreType.DMA((depth,)),
            pltpu.SemaphoreType.DMA,
            pltpu.SemaphoreType.DMA((depth,)),
            pltpu.SemaphoreType.DMA,
            pltpu.SemaphoreType.DMA((depth,)),
            pltpu.SemaphoreType.REGULAR,
        ],
        compiler_params=pltpu.CompilerParams(
            collective_id=0, has_side_effects=True, vmem_limit_bytes=40 << 20
        ),
        name="exchange_fit",
    )(*operands)
    results = (updates, standardized, norm)
    updates, standardized, norm = pl.pallas_call(
        release,
        out_shape=tuple(jax.ShapeDtypeStruct(r.shape, r.dtype) for r in results),
        in_specs=[vmem] * 3,
        out_specs=[pl.BlockSpec(memory_space=pltpu.HBM)] * 3,
        scratch_shapes=[pltpu.SemaphoreType.DMA((3,))],
        compiler_params=pltpu.CompilerParams(vmem_limit_bytes=4 << 20),
        name="release",
    )(*results)
    standardized = standardized.reshape(n, width)[:, :block_rows] if width != block_rows else standardized
    return (updates, standardized.reshape(row_count), norm[0, 0])


def solution(mesh):
    in_specs = (
        P(("grp", "dev")),
        P(("grp", "dev")),
        P(),
        P(("grp", "dev")),
        P(None, ("grp", "dev")),
        P(("grp", "dev")),
        P(("grp", "dev")),
        P(None, ("grp", "dev")),
    )
    out_specs = (P(None, ("grp", "dev")), P(("grp", "dev")), P())
    return jax.shard_map(body, mesh=mesh, in_specs=in_specs, out_specs=out_specs, check_vma=False)
```

```python
import functools

import jax
import jax.numpy as jnp
from jax import lax
from jax.experimental import pallas as pl
from jax.experimental.pallas import tpu as pltpu
from jax.sharding import PartitionSpec as P

LANES = 128
SUBLANES = 8
CORES = 2
MESH = pl.DeviceIdType.MESH


def solve_rows(normal, moments):
    params = len(moments)
    factor = {}
    inverse = []
    for column in range(params):
        running = normal[column][column]
        for earlier in range(column):
            running = running - factor[column, earlier] ** 2
        inverse.append(1.0 / jnp.sqrt(running))
        for target in range(column + 1, params):
            current = normal[target][column]
            for earlier in range(column):
                current = current - factor[target, earlier] * factor[column, earlier]
            factor[target, column] = current * inverse[column]
    forward = []
    for target in range(params):
        current = moments[target]
        for earlier in range(target):
            current = current - factor[target, earlier] * forward[earlier]
        forward.append(current * inverse[target])
    backward = [None] * params
    for target in reversed(range(params)):
        current = forward[target]
        for later in range(target + 1, params):
            current = current - factor[later, target] * backward[later]
        backward[target] = current * inverse[target]
    return backward


def thirds(values):
    high = values.astype(jnp.bfloat16)
    rest = values - high.astype(jnp.float32)
    middle = rest.astype(jnp.bfloat16)
    last = (rest - middle.astype(jnp.float32)).astype(jnp.bfloat16)
    return jnp.concatenate([high, middle, last], axis=0)


def gather_lanes(table, index):
    return jnp.take_along_axis(table, index, axis=1, mode="promise_in_bounds")


def kernel(
    sizes,
    source_hbm, slot_hbm, owner_hbm, counts_hbm, partials_hbm, residual_hbm, weight_hbm, prior_hbm,
    updates_ref, fresh_ref, norm_ref,
    source_ref, slot_ref, owner_ref, counts_ref, partials_ref, residual_ref, weight_ref, prior_ref,
    root_buf, cell_buf, place_buf, out_buf, in_buf, meta_buf, first_buf, room_buf, sums_buf, tables,
    load_sem, send_sem, recv_sem, meta_send_sem, meta_recv_sem, sums_send_sem, sums_recv_sem,
    table_send_sem, table_recv_sem, gate_sem,
):
    groups, members, width, pad_slots = sizes
    n = groups * members
    params = partials_ref.shape[0]
    words = params + 2
    items = params + 1
    depth = members // CORES
    plane = groups * CORES
    pieces = width // LANES
    low = 2 if groups % 2 == 0 else 1
    high = groups // low
    row_pairs = (
        (owner_hbm, owner_ref), (source_hbm, source_ref), (slot_hbm, slot_ref), (weight_hbm, weight_ref),
        (residual_hbm, residual_ref), (partials_hbm, partials_ref), (counts_hbm, counts_ref), (prior_hbm, prior_ref),
    )
    loads = [pltpu.make_async_copy(a, b, load_sem.at[i]) for i, (a, b) in enumerate(row_pairs)]
    for load in loads:
        load.start()
    my_group, my_member = lax.axis_index("grp"), lax.axis_index("dev")
    my_depth, my_core = my_member // CORES, my_member % CORES
    me = my_group * members + my_member
    my_seat = my_group * CORES + my_core

    def target(step):
        jump = step // CORES
        group = (my_group // low + jump // low) % high * low + (my_group % low + jump % low) % low
        return group, (my_core + step % CORES) % CORES

    def origin(step):
        jump = step // CORES
        group = (my_group // low + high - jump // low) % high * low + (my_group % low + low - jump % low) % low
        return group, (my_core + CORES - step % CORES) % CORES

    def seat_coords(seat):
        group, core = seat
        return (group, my_depth * CORES + core)

    def level_coords(level, core=None):
        return (my_group, level * CORES + (my_core if core is None else core))

    lead = CORES - 1

    def level_at(turn):
        return depth - 1 - turn

    def unit_of(index):
        return level_at(index // CORES * CORES + my_core), index % CORES

    def home_of(level, core):
        turn = depth - 1 - level
        return turn % CORES, turn // CORES * CORES + core

    def far_first(step):
        return jnp.where(my_depth < depth // 2, depth - 1 - step, step)

    barrier = pltpu.get_barrier_semaphore()
    few = depth <= 4
    used = 3 * SUBLANES - 2

    def tell(semaphore, level):
        for core in range(CORES):
            pl.semaphore_signal(semaphore, inc=1, device_id=level_coords(level, core), device_id_type=MESH)

    def greet_level(step, carry):
        level = level_at(step)
        pl.when(level > my_depth)(lambda: tell(barrier, level))
        return carry

    for step in range(plane - 1, 0, -1):
        pl.semaphore_signal(barrier, inc=1, device_id=seat_coords(target(step)), device_id_type=MESH)
    lax.fori_loop(0, depth, greet_level, 0, unroll=few)

    for load in loads:
        load.wait()

    meta_buf[my_core * depth + my_depth] = jnp.concatenate(
        [prior_ref[...], counts_ref[...].astype(jnp.float32), jnp.zeros((SUBLANES - items, LANES), jnp.float32)], axis=0
    )
    root = jnp.sqrt(weight_ref[...])
    root_buf[...] = root
    residual_ref[...] = residual_ref[...] * root
    cell_buf[...] = (source_ref[...] * pad_slots + slot_ref[...]).astype(jnp.float32)

    sublane = lax.broadcasted_iota(jnp.int32, (SUBLANES, LANES), 0)

    def prepare(level, seat, carry):
        k = seat // CORES * members + level * CORES + seat % CORES
        for piece in range(pieces):
            row = pl.ds(k * pieces + piece, 1)
            cols = pl.ds(pl.multiple_of(k * width + piece * LANES, LANES), LANES)

            def spread(ref):
                return jnp.broadcast_to(ref[row, :], (SUBLANES, LANES))

            scaled = partials_ref[:, cols] * jnp.broadcast_to(root_buf[row, :], (params, LANES))
            part = slice(piece * LANES, (piece + 1) * LANES)
            out_buf[k, 0:params, part] = scaled
            out_buf[k, params:items, part] = residual_ref[row, :]
            out_buf[k, items:words, part] = cell_buf[row, :]
            out_buf[k, words : words + 1, part] = slot_ref[row, :].astype(jnp.float32)
        return carry

    def prepare_level(level, carry):
        return lax.fori_loop(0, plane, functools.partial(prepare, level), carry, unroll=2)

    prepare_level(level_at(0), 0)

    pl.semaphore_wait(barrier, plane - 1 + CORES * my_depth)

    def meta_copy(level, core):
        slot = my_core * depth + my_depth
        return pltpu.make_async_remote_copy(
            src_ref=meta_buf.at[slot], dst_ref=meta_buf.at[slot], send_sem=meta_send_sem,
            recv_sem=meta_recv_sem.at[my_depth], device_id=level_coords(level, core), device_id_type=MESH,
        )

    def row_copy(level, core, jump, part):
        home, unit = home_of(level, core)
        group, _ = target(jump * CORES)
        return pltpu.make_async_remote_copy(
            src_ref=out_buf.at[group * members + level * CORES + core, pl.ds(0, words)],
            dst_ref=in_buf.at[unit, my_seat, pl.ds(0, words)],
            send_sem=send_sem, recv_sem=recv_sem.at[unit, part],
            device_id=seat_coords((group, home)), device_id_type=MESH,
        )

    def sums_copy(level, stage, core):
        slot = core * depth + my_depth
        return pltpu.make_async_remote_copy(
            src_ref=sums_buf.at[slot, stage, pl.ds(0, used)], dst_ref=sums_buf.at[slot, stage, pl.ds(0, used)],
            send_sem=sums_send_sem, recv_sem=sums_recv_sem.at[stage],
            device_id=level_coords(level, lead), device_id_type=MESH,
        )

    def table_copy(stage, seat):
        pair = pl.ds(my_group * members + stage * CORES, CORES)
        return pltpu.make_async_remote_copy(
            src_ref=tables.at[pair], dst_ref=tables.at[pair],
            send_sem=table_send_sem, recv_sem=table_recv_sem.at[stage],
            device_id=seat_coords(seat), device_id_type=MESH,
        )

    def send_meta_down(level, carry):
        for core in range(CORES):
            remote = jnp.logical_or(level < my_depth, jnp.logical_and(level == my_depth, my_core != core))
            pl.when(remote)(meta_copy(level, core).start)
        pl.when(level < my_depth)(lambda: tell(gate_sem, level))
        return carry

    def send_meta_up(step, carry):
        level = level_at(step)
        for core in range(CORES):
            pl.when(level > my_depth)(meta_copy(level, core).start)
        return carry

    lax.fori_loop(0, depth, send_meta_down, 0, unroll=few)
    batches = ([0] + list(range(groups - 1, 1, -1)), [1])

    def send_rows(level):
        for core in range(CORES):
            for jump in range(groups - 1, -1, -1):
                copy = row_copy(level, core, jump, int(jump in batches[1]))
                if jump:
                    copy.start()
                else:
                    pl.when(home_of(level, core)[0] != my_core)(copy.start)

    def stream_rows(turn, carry):
        prepare_level(level_at(turn), 0)
        send_rows(level_at(turn - 1))
        return carry

    lax.fori_loop(1, depth, stream_rows, 0)
    send_rows(level_at(depth - 1))

    def own_rows(unit, carry):
        level, core = unit_of(unit)
        in_buf[unit, my_seat] = out_buf[my_group * members + level * CORES + core]
        return carry

    lax.fori_loop(0, depth, own_rows, 0)

    src_local = counts_ref.shape[1]
    square = (src_local, LANES)
    row_index = lax.broadcasted_iota(jnp.int32, square, 0)
    lane_index = lax.broadcasted_iota(jnp.int32, square, 1)
    diagonal = row_index == lane_index
    spare = 4

    def invert(unit, carry):
        level, core = unit_of(unit)
        position = (my_group * members + level * CORES + core) * src_local + row_index

        def scan(step, total):
            for part in range(spare):
                tile = step * spare + part
                total = jnp.where(owner_ref[pl.ds(tile, 1), :] == position, tile * LANES + lane_index, total)
            return total

        found = lax.fori_loop(0, owner_ref.shape[0] // spare, scan, jnp.zeros(square, jnp.int32))
        source_at = jnp.sum(found.astype(jnp.float32), axis=1, keepdims=True)
        first_buf[unit] = jnp.broadcast_to(source_at * pad_slots, square).astype(jnp.int32)
        return carry

    lax.fori_loop(0, depth, invert, 0)

    @pl.when(my_depth < depth - 1)
    def open_up():
        pl.semaphore_wait(gate_sem, CORES * (depth - 1 - my_depth))
        lax.fori_loop(0, depth, send_meta_up, 0, unroll=few)

    batch = min(32, owner_ref.shape[0])

    def locate(step, carry):
        rows = pl.ds(pl.multiple_of(step * SUBLANES, SUBLANES), SUBLANES)
        source = source_ref[rows, :]
        lane, tile = source % LANES, source // LANES

        def look(group, found):
            for t in range(batch):
                row = group * batch + t
                entry = jnp.broadcast_to(owner_ref[pl.ds(row, 1), :], (SUBLANES, LANES))
                found = jnp.where(tile == row, gather_lanes(entry, lane), found)
            return found

        found = jnp.full((SUBLANES, LANES), -1, jnp.int32)
        if owner_ref.shape[0] == batch:
            found = look(0, found)
        else:
            found = lax.fori_loop(0, owner_ref.shape[0] // batch, look, found)
        place_buf[rows, :] = found % LANES
        return carry

    lax.fori_loop(0, source_ref.shape[0] // SUBLANES, locate, 0)


    others = pl.ds(0, CORES * depth - 1)

    def await_meta(level):
        def take(count):
            block = meta_buf.at[pl.ds(0, count)]
            pltpu.make_async_remote_copy(
                src_ref=block, dst_ref=block, send_sem=meta_send_sem, recv_sem=meta_recv_sem.at[level],
                device_id=seat_coords(target(1)), device_id_type=MESH,
            ).wait_recv()

        pl.when(level == my_depth)(lambda: take(CORES - 1))
        pl.when(level != my_depth)(lambda: take(CORES))

    def find_room(unit, carry):
        level, core = unit_of(unit)
        counts = meta_buf[core * depth + level, params:items, :]
        counts = jnp.sum(jnp.where(diagonal, counts, 0.0), axis=1, keepdims=True)
        room_buf[unit] = jnp.broadcast_to(counts, square).astype(jnp.int32).astype(jnp.uint32)
        return carry

    wide_sublane = lax.broadcasted_iota(jnp.int32, (SUBLANES, width), 0)

    low_rows = wide_sublane < 2
    sixth_row = wide_sublane == items
    outer_rows = jnp.logical_or(wide_sublane == 0, wide_sublane >= items)

    def absorb(unit, slot, sign):
        first_cell, room = first_buf[unit], room_buf[unit]
        rows = in_buf[unit, slot]

        def spread(i):
            return jnp.broadcast_to(in_buf[unit, slot, i : i + 1, :], (SUBLANES, width))

        hot = []
        for piece in range(pieces):
            part = in_buf[unit, slot, items:words, piece * LANES : (piece + 1) * LANES].astype(jnp.int32)
            hit = (part - first_cell).astype(jnp.uint32) < room
            hot.append(jnp.where(hit, sign, 0.0))
        hot = jnp.concatenate(hot, axis=1).astype(jnp.bfloat16)
        products = jnp.concatenate(
            [
                jnp.where(sixth_row, spread(5), spread(0)) * jnp.where(sixth_row, pltpu.roll(rows, 1, 0), rows),
                jnp.where(outer_rows, spread(3), spread(1)) * jnp.where(outer_rows, pltpu.roll(rows, 3, 0), rows),
                jnp.where(low_rows, spread(4), spread(2)) * jnp.where(low_rows, pltpu.roll(rows, 4, 0), rows),
                jnp.zeros((SUBLANES, width), jnp.float32),
            ],
            axis=0,
        )
        return lax.dot_general(
            thirds(products), hot, (((1,), (1,)), ((), ())), preferred_element_type=jnp.float32
        )

    height = 4 * SUBLANES

    def gather_unit(unit, carry):
        level, owner_core = unit_of(unit)
        totals = [None, None]
        for part, jumps in enumerate(batches):
            count = CORES * len(jumps) - (part == 0)
            block = in_buf.at[unit, pl.ds(0, count), pl.ds(0, words)]
            pltpu.make_async_remote_copy(
                src_ref=block, dst_ref=block, send_sem=send_sem, recv_sem=recv_sem.at[unit, part],
                device_id=seat_coords(target(1)), device_id_type=MESH,
            ).wait_recv()
            for jump in jumps:
                group, _ = origin(jump * CORES)
                for core in range(CORES):
                    part_sum = absorb(unit, group * CORES + core, 1.0 - 2.0 * core)
                    totals[core] = part_sum if totals[core] is None else totals[core] + part_sum
        total = totals[0] - totals[1]
        total = total[0:height] + total[height : 2 * height] + total[2 * height : 3 * height]
        sums_buf[owner_core * depth + my_depth, level] = total[0 : 3 * SUBLANES]

        def send_sums(step, carry):
            aim = far_first(step)
            pl.when(jnp.logical_or(aim != my_depth, my_core != lead))(sums_copy(aim, level, owner_core).start)
            return carry

        lax.fori_loop(0, depth, send_sums, 0, unroll=few)
        return carry

    def gather_turn(turn, carry):
        await_meta(unit_of(turn * CORES)[0])
        lax.fori_loop(turn * CORES, (turn + 1) * CORES, find_room, 0)
        return lax.fori_loop(turn * CORES, (turn + 1) * CORES, gather_unit, carry)

    def other_meta(turn, carry):
        await_meta(level_at(turn * CORES + 1 - my_core))
        return carry

    lax.fori_loop(0, depth // CORES, gather_turn, 0)
    lax.fori_loop(0, depth // CORES, other_meta, 0)
    at = {(0, 0): 0, (0, 1): 1, (0, 2): 2, (0, 3): 3, (0, 4): 4, (0, 5): 5, (5, 5): 6,
          (3, 5): 8, (1, 1): 9, (1, 2): 10, (1, 3): 11, (1, 4): 12, (1, 5): 13, (3, 3): 14, (3, 4): 15,
          (4, 4): 16, (4, 5): 17, (2, 2): 18, (2, 3): 19, (2, 4): 20, (2, 5): 21}

    def fit_level(level, count):
        block = sums_buf.at[pl.ds(0, count), level, pl.ds(0, used)]
        pltpu.make_async_remote_copy(
            src_ref=block, dst_ref=block, send_sem=sums_send_sem, recv_sem=sums_recv_sem.at[level],
            device_id=level_coords((my_depth + 1) % depth), device_id_type=MESH,
        ).wait_recv()
        for core in range(CORES):
            fit(level, core)
        for step in range(plane - 1, 0, -1):
            table_copy(level, target(step)).start()

    def fit(level, core):
        def gather_sums(slot, total):
            return total + sums_buf[core * depth + slot, level, 0:used, :]

        total = lax.fori_loop(1, depth, gather_sums, sums_buf[core * depth, level, 0:used, :], unroll=few)
        meta = meta_buf[core * depth + level]

        def entry(i, j):
            spot = at[min(i, j), max(i, j)]
            return total[spot : spot + 1, :]

        normal = [[entry(i, j) for j in range(params)] for i in range(params)]
        moments = [entry(i, params) for i in range(params)]
        with_prior = [[normal[i][j] for j in range(params)] for i in range(params)]
        for i in range(params):
            with_prior[i][i] = normal[i][i] + meta[i : i + 1, :]
        updates = solve_rows(with_prior, moments)
        squares = entry(params, params)
        for i in range(params):
            fitted = normal[i][0] * updates[0]
            for j in range(1, params):
                fitted = fitted + normal[i][j] * updates[j]
            squares = squares + updates[i] * (fitted - 2.0 * moments[i])
        minus = jnp.full((1, LANES), -1.0, jnp.float32)
        tables[my_group * members + level * CORES + core] = jnp.concatenate(
            updates + [minus, squares, meta[params:items, :]], axis=0
        )

    @pl.when(my_core == lead)
    def lead_fits():
        def fit_pair(step, carry):
            for core in range(CORES):
                fit_level(level_at(step * CORES + core), CORES * (depth - (core == lead)))
            return carry

        lax.fori_loop(0, depth // CORES, fit_pair, 0)

    def drain(ref, semaphore):
        pltpu.make_async_remote_copy(
            src_ref=ref, dst_ref=ref, send_sem=semaphore, recv_sem=meta_recv_sem.at[0],
            device_id=seat_coords(target(1)), device_id_type=MESH,
        ).wait_send()

    def refit_level(turn, tails):
        level = level_at(turn)

        def await_tables(count):
            pairs = pl.ds(0, count * CORES)
            pltpu.make_async_remote_copy(
                src_ref=tables.at[pairs], dst_ref=tables.at[pairs],
                send_sem=table_send_sem, recv_sem=table_recv_sem.at[level],
                device_id=seat_coords(target(1)), device_id_type=MESH,
            ).wait_recv()

        @pl.when(my_core == lead)
        def await_leads():
            await_tables(groups - 1)

        @pl.when(my_core != lead)
        def await_all():
            await_tables(groups)

        for seat in range(plane):
            k = seat // CORES * members + level * CORES + seat % CORES
            table = tables[k]
            tails = tails + table[items : words + 1, :]
            for piece in range(pieces):
                row = pl.ds(k * pieces + piece, 1)
                place = jnp.broadcast_to(place_buf[row, :], (SUBLANES, LANES))
                picked = gather_lanes(table, place)
                rows = out_buf[k, :, piece * LANES : (piece + 1) * LANES]
                fresh = -jnp.sum(jnp.where(sublane < items, picked * rows, 0.0), axis=0, keepdims=True)
                live = rows[words : words + 1, :] < picked[words : words + 1, :]
                root_buf[row, :] = jnp.where(live, fresh, 0.0)
        return tails

    tails = lax.fori_loop(0, depth - 1, refit_level, jnp.zeros((2, LANES), jnp.float32))
    sent = depth * (plane - 1)
    drain(out_buf.at[pl.ds(0, sent), pl.ds(0, words)], send_sem)
    drain(meta_buf.at[others], meta_send_sem)

    @pl.when(my_core == lead)
    def drain_lead():
        drain(sums_buf.at[pl.ds(0, depth - 1), :, pl.ds(0, used)], sums_send_sem)

    @pl.when(my_core != lead)
    def drain_follower():
        drain(sums_buf.at[pl.ds(0, depth), :, pl.ds(0, used)], sums_send_sem)

    tails = refit_level(depth - 1, tails)
    tails = jnp.sum(tails, axis=1, keepdims=True)
    updates_ref[...] = tables[me, 0:params, :]
    norm = jnp.sqrt(jnp.maximum(tails[0:1], 0.0) / tails[1:2] + 1e-06)
    norm_ref[...] = jnp.broadcast_to(norm, norm_ref.shape)
    scale = 1.0 / norm
    fresh_ref[...] = root_buf[...] * scale

    @pl.when(my_core == lead)
    def drain_tables():
        def drain_seat(step, carry):
            drain(tables.at[pl.ds(0, depth * CORES)], table_send_sem)
            return carry

        lax.fori_loop(1, plane, drain_seat, 0)


def release(a_ref, b_ref, c_ref, a_out, b_out, c_out, sem):
    pairs = ((a_ref, a_out), (b_ref, b_out), (c_ref, c_out))
    copies = [pltpu.make_async_copy(x, y, sem.at[i]) for i, (x, y) in enumerate(pairs)]
    for copy in copies:
        copy.start()
    for copy in copies:
        copy.wait()


def body(source_id, slot, owner, counts, partials, residual, weight, prior):
    groups, members = lax.axis_size("grp"), lax.axis_size("dev")
    n = groups * members
    params = partials.shape[0]
    row_count = residual.shape[0]
    src_local = counts.shape[0]
    block_rows = row_count // n
    width = -(-block_rows // LANES) * LANES
    depth, plane = members // CORES, groups * CORES

    def lay(array, fill):
        if width == block_rows:
            return array
        blocks = array.reshape(-1, n, block_rows)
        blocks = jnp.pad(blocks, ((0, 0), (0, 0), (0, width - block_rows)), constant_values=fill)
        return blocks.reshape(array.shape[:-1] + (n * width,))

    def dense(array, fill):
        return lay(array, fill).reshape(-1, LANES)

    vmem = pl.BlockSpec(memory_space=pltpu.VMEM)
    operands = (
        dense(source_id, -1),
        dense(slot, 0),
        owner.reshape(-1, LANES),
        counts.reshape(1, src_local),
        lay(partials, 0),
        dense(residual, 0),
        dense(weight, 1),
        prior,
    )
    operands = tuple(pltpu.with_memory_space_constraint(x, pltpu.HBM) for x in operands)
    rows = n * width // LANES
    updates, standardized, norm = pl.pallas_call(
        functools.partial(kernel, (groups, members, width, row_count // src_local)),
        out_shape=(
            pltpu.VMEM((params, src_local), jnp.float32),
            pltpu.VMEM((rows, LANES), jnp.float32),
            pltpu.VMEM((1, LANES), jnp.float32),
        ),
        in_specs=[pl.BlockSpec(memory_space=pltpu.HBM)] * len(operands),
        out_specs=(vmem, vmem, vmem),
        scratch_shapes=[pltpu.VMEM(operand.shape, operand.dtype) for operand in operands] + [
            pltpu.VMEM((rows, LANES), jnp.float32),
            pltpu.VMEM((rows, LANES), jnp.float32),
            pltpu.VMEM((rows, LANES), jnp.int32),
            pltpu.VMEM((n, SUBLANES, width), jnp.float32),
            pltpu.VMEM((depth, plane, SUBLANES, width), jnp.float32),
            pltpu.VMEM((CORES * depth, SUBLANES, LANES), jnp.float32),
            pltpu.VMEM((depth, src_local, LANES), jnp.int32),
            pltpu.VMEM((depth, src_local, LANES), jnp.uint32),
            pltpu.VMEM((CORES * depth, depth, 3 * SUBLANES, LANES), jnp.float32),
            pltpu.VMEM((n, SUBLANES, LANES), jnp.float32),
            pltpu.SemaphoreType.DMA((len(operands),)),
            pltpu.SemaphoreType.DMA,
            pltpu.SemaphoreType.DMA((depth, 2)),
            pltpu.SemaphoreType.DMA,
            pltpu.SemaphoreType.DMA((depth,)),
            pltpu.SemaphoreType.DMA,
            pltpu.SemaphoreType.DMA((depth,)),
            pltpu.SemaphoreType.DMA,
            pltpu.SemaphoreType.DMA((depth,)),
            pltpu.SemaphoreType.REGULAR,
        ],
        compiler_params=pltpu.CompilerParams(
            collective_id=0, has_side_effects=True, vmem_limit_bytes=40 << 20
        ),
        name="exchange_fit",
    )(*operands)
    results = (updates, standardized, norm)
    updates, standardized, norm = pl.pallas_call(
        release,
        out_shape=tuple(jax.ShapeDtypeStruct(r.shape, r.dtype) for r in results),
        in_specs=[vmem] * 3,
        out_specs=[pl.BlockSpec(memory_space=pltpu.HBM)] * 3,
        scratch_shapes=[pltpu.SemaphoreType.DMA((3,))],
        compiler_params=pltpu.CompilerParams(vmem_limit_bytes=4 << 20),
        name="release",
    )(*results)
    standardized = standardized.reshape(n, width)[:, :block_rows] if width != block_rows else standardized
    return (updates, standardized.reshape(row_count), norm[0, 0])


def solution(mesh):
    in_specs = (
        P(("grp", "dev")),
        P(("grp", "dev")),
        P(),
        P(("grp", "dev")),
        P(None, ("grp", "dev")),
        P(("grp", "dev")),
        P(("grp", "dev")),
        P(None, ("grp", "dev")),
    )
    out_specs = (P(None, ("grp", "dev")), P(("grp", "dev")), P())
    return jax.shard_map(body, mesh=mesh, in_specs=in_specs, out_specs=out_specs, check_vma=False)
```
